32 devices in a mesh: row: 16 (over z, y, core), col: 2 (over x).
Axes of the slice: x: 2, y: 2, z: 4, core: 2. Of those that a mesh axis runs over, the one named last changes fastest.
Arguments:
- positions: float32 [3, 8192], P(None, ('row', 'col')), as said below
- velocities: float32 [3, 8192], P(None, ('row', 'col')), may hold values from -6 to 6
- old_forces: float32 [3, 8192], P(None, ('row', 'col')), may hold values from -6 to 6
- charges: float32 [8192], P(('row', 'col')), may hold values from -3 to 3
- atom_types: int32 [8192], P(('row', 'col')), may hold values from 0 to 7
- type_table: float32 [7, 8], replicated, may hold values from 0.003 to 2, as said below
- tile_pairs: int32 [16, 2, 2, 32], P('row', 'col'), may hold values from -1 to 31, as said below
Outputs:
- new_positions: float32 [3, 8192], P(None, ('row', 'col'))
- new_velocities: float32 [3, 8192], P(None, ('row', 'col'))
- new_forces: float32 [3, 8192], P(None, ('row', 'col'))
The draws below stay inside these ranges and needn't reach their ends.
Inputs may be any that keep to these rules, and one draw needn't show every extreme that they name: `positions`: the atoms of one block lie together in a cube of its own; the blocks' cubes fill a cubic lattice in the order of the block numbers, at about 0.1 atoms per cubic angstrom. `tile_pairs`: on each device the first n slots hold distinct pairs (a, g) with a below 4 and g below 32, each a tile whose blocks' cubes lie within 12 angstrom of each other; the other slots hold -1 in both entries. n is at most 32, differs from device to device, and equals 32 on the device with the most such tiles when it has 32 or more; the list is a sampled part of each device's near tiles, not all of them. `type_table`: Rows: intrinsic radii 1 to 2, screening scales 0.15 to 0.6, neck weights 0.003 to 0.012, alpha 0.6 to 1, beta 0.3 to 0.9, gamma 0.2 to 0.6, masses 0.5 to 2.
All inputs are finite; a program needn't handle non-finite values.
Results may differ from the reference program's by a relative error of at most 0.0003.
Values sent between devices are 32-bit elements; how exact they have to be, the bound alone decides.
A program may use at most 64 MiB of HBM per device.

```python
import math
import jax
import jax.numpy as jnp
from jax import lax

TILE = 128
BLK_DEV = 2
TILE_CAP = 32
TYPES = 8
ATOMS = 8192
I_BLOCKS = 4
N_ROW = 16
N_COL = 2


def block_frame():
    block_total = ATOMS // TILE
    lattice_side = int(math.ceil(block_total ** (1.0 / 3.0) - 1e-09))
    if lattice_side ** 3 < block_total:
        lattice_side = lattice_side + 1
    cube_edge = (TILE * 10.0) ** (1.0 / 3.0)
    block_ids = jnp.arange(block_total, dtype=jnp.int32)
    lattice = jnp.stack([block_ids // (lattice_side * lattice_side), block_ids // lattice_side % lattice_side, block_ids % lattice_side], axis=0)
    return (lattice.astype(jnp.float32) * cube_edge, cube_edge)


def draw_positions(key, part):
    corners, cube_edge = block_frame()
    unit = jax.random.uniform(jax.random.fold_in(key, 21), (3, ATOMS), jnp.float32)
    return (jnp.repeat(corners, TILE, axis=1) + cube_edge * unit).astype(jnp.float32)


def draw_type_table(key, part):
    lowest = jnp.array([1.0, 0.15, 0.003, 0.6, 0.3, 0.2, 0.5], jnp.float32)[:, None]
    highest = jnp.array([2.0, 0.6, 0.012, 1.0, 0.9, 0.6, 2.0], jnp.float32)[:, None]
    in_logs = jnp.array([1.0, 1.0, 1.0, 0.0, 0.0, 0.0, 1.0], jnp.float32)[:, None]
    unit = jax.random.uniform(jax.random.fold_in(key, 5), (7, TYPES), jnp.float32)
    linear = lowest + (highest - lowest) * unit
    logged = jnp.exp(jnp.log(lowest) + (jnp.log(highest) - jnp.log(lowest)) * unit)
    return (in_logs * logged + (1.0 - in_logs) * linear).astype(jnp.float32)


def draw_tile_pairs(key, part):
    devices_all = N_ROW * N_COL
    i_count = BLK_DEV * N_COL
    j_count = BLK_DEV * N_ROW
    combos = i_count * j_count
    corners, cube_edge = block_frame()
    row_ids = jnp.arange(N_ROW, dtype=jnp.int32)[:, None, None]
    col_ids = jnp.arange(N_COL, dtype=jnp.int32)[None, :, None]
    local_i = jnp.arange(i_count, dtype=jnp.int32)[None, None, :]
    local_j = jnp.arange(j_count, dtype=jnp.int32)[None, None, :]
    global_i = row_ids * i_count + local_i + 0 * col_ids
    global_j = (local_j // BLK_DEV * N_COL + col_ids) * BLK_DEV + local_j % BLK_DEV + 0 * row_ids
    corner_i = jnp.take(corners, global_i.reshape(-1), axis=1).reshape(3, N_ROW, N_COL, i_count)
    corner_j = jnp.take(corners, global_j.reshape(-1), axis=1).reshape(3, N_ROW, N_COL, j_count)
    apart = jnp.abs(corner_i[:, :, :, :, None] - corner_j[:, :, :, None, :])
    gap = jnp.maximum(apart - cube_edge - 0.001, 0.0)
    near = (jnp.sum(gap * gap, axis=0) < 144.0).reshape(devices_all, combos)
    key_list = jax.random.split(jax.random.fold_in(key, 11), devices_all)
    ranks = jax.vmap(lambda subkey: jax.random.permutation(subkey, combos))(key_list).astype(jnp.int32)
    score = jnp.where(near, ranks + 1, 0)
    chosen_score, chosen = lax_top(score)
    near_count = jnp.sum(near.astype(jnp.int32), axis=1)
    fewest = (TILE_CAP + 7) // 8
    level_count = 64
    skew_level = jax.random.randint(jax.random.fold_in(key, 12), (devices_all,), 0, level_count + 1)
    live_count = fewest + (TILE_CAP - fewest) * skew_level * skew_level * skew_level // (level_count * level_count * level_count)
    busiest = jnp.argmax(near_count)
    live_count = jnp.where(jnp.arange(devices_all) == busiest, TILE_CAP, live_count)
    live_count = jnp.minimum(live_count, near_count)
    slot_ids = jnp.arange(TILE_CAP)[None, :]
    live_slot = slot_ids < live_count[:, None]
    first_ids = jnp.where(live_slot, chosen // j_count, -1)
    second_ids = jnp.where(live_slot, chosen % j_count, -1)
    stacked = jnp.stack([first_ids, second_ids], axis=1)
    return stacked.reshape(N_ROW, N_COL, 2, TILE_CAP).astype(jnp.int32)


def lax_top(score):
    return jax.lax.top_k(score, TILE_CAP)


def plant(result, key, smallest, top_value):
    spot = [jax.random.randint(jax.random.fold_in(key, axis), (), 0, length) for axis, length in enumerate(result.shape)]
    longest = result.shape.index(max(result.shape))
    beside = spot[:longest] + [(spot[longest] + 1) % result.shape[longest]] + spot[longest + 1:]
    return result.at[tuple(spot)].set(smallest).at[tuple(beside)].set(top_value)


def levels(key, dims, cuts, least, largest):
    level = 1.0
    for position, blocks in cuts:
        steps = jax.random.uniform(jax.random.fold_in(jax.random.fold_in(key, 6), position), (blocks,), jnp.float32, least / len(cuts), largest / len(cuts))
        level = level * jnp.repeat(jnp.exp(steps), dims[position] // blocks).reshape((-1,) + (1,) * (len(dims) - 1 - position))
    return level


def scatter_about(key, dims, spread, bound, cuts=(), held_as=jnp.bfloat16):
    result = jax.random.normal(key, dims, jnp.float32) * spread
    if len(cuts) > 0:
        result = levels(key, dims, cuts, -0.22, 0.18) * result
    return jnp.clip(result, min=-bound, max=bound).astype(held_as)


def setup_inputs(seed: int = 0) -> dict:
    keys = jax.random.split(jax.random.key(seed), 8)
    return {
        "positions": draw_positions(jax.random.fold_in(keys[7], 71), 0),
        "velocities": scatter_about(keys[1], (3, ATOMS), 1.0, 6.0, ((1, 32),), jnp.float32),
        "old_forces": scatter_about(keys[2], (3, ATOMS), 1.0, 6.0, ((1, 32),), jnp.float32),
        "charges": scatter_about(keys[3], (ATOMS,), 0.5, 3.0, ((0, 32),), jnp.float32),
        "atom_types": plant(jax.random.randint(keys[4], (ATOMS,), 0, TYPES), jax.random.fold_in(keys[4], 1), 0, TYPES - 1).astype(jnp.int32),
        "type_table": draw_type_table(jax.random.fold_in(keys[7], 71), 0),
        "tile_pairs": draw_tile_pairs(jax.random.fold_in(keys[7], 71), 0),
    }


CUTOFF = 12.0
COULOMB = 32.0
TIMESTEP = 0.5
OFFSET = 0.09
NECK_GAP = 0.5
NECK_WIDTH = 16.0

def taper(dist_sq):
    taper_base = jnp.maximum(1.0 - dist_sq / (CUTOFF * CUTOFF), 0.0)
    return (taper_base * taper_base, -2.0 * taper_base / (CUTOFF * CUTOFF))

def screening(dist_sq, intrinsic, other_radius, other_scale, other_neck):
    soft_sq = dist_sq + intrinsic * intrinsic
    neck_gap = intrinsic + other_radius + NECK_GAP
    neck_off = dist_sq - neck_gap * neck_gap
    neck_bump = jnp.exp(-neck_off * neck_off / NECK_WIDTH)
    volume = other_scale * other_radius * other_radius * other_radius
    descreen = volume / (soft_sq * soft_sq) + other_neck * neck_bump
    slope = -2.0 * volume / (soft_sq * soft_sq * soft_sq) - other_neck * neck_bump * neck_off * (2.0 / NECK_WIDTH)
    weight, w_slope = taper(dist_sq)
    return (weight * descreen, w_slope * descreen + weight * slope)

def separation(coords_i, coords_j):
    offset_vec = coords_i[:, :, :, None] - coords_j[:, :, None, :]
    return (offset_vec, lax.optimization_barrier(jnp.sum(offset_vec * offset_vec, axis=1)))

def born_terms(side_i, side_j, mask):
    offset_vec, dist_sq = separation(side_i[:, 0:3], side_j[:, 0:3])
    value, slope = screening(dist_sq, side_i[:, 4][:, :, None], side_j[:, 4][:, None, :], side_j[:, 5][:, None, :], side_j[:, 6][:, None, :])
    return lax.optimization_barrier(jnp.sum(mask * value, axis=2))[:, None, :]

def pair_terms(side_i, side_j, mask):
    offset_vec, dist_sq = separation(side_i[:, 0:3], side_j[:, 0:3])
    charge_pair = side_i[:, 3][:, :, None] * side_j[:, 3][:, None, :]
    radius_j = side_j[:, -1][:, None, :]
    radii_prod = side_i[:, -1][:, :, None] * radius_j
    radii_exp = jnp.exp(-dist_sq / (4.0 * radii_prod))
    inv_eff = 1.0 / jnp.sqrt(dist_sq + radii_prod * radii_exp)
    inv_cube = inv_eff * inv_eff * inv_eff
    weight, w_slope = taper(dist_sq)
    d_dist = mask * charge_pair * (w_slope * inv_eff - 0.5 * weight * (1.0 - 0.25 * radii_exp) * inv_cube)
    d_radius = mask * -0.5 * weight * charge_pair * inv_cube * radii_exp * (1.0 + dist_sq / (4.0 * radii_prod)) * radius_j
    direct = 2.0 * COULOMB * lax.optimization_barrier(jnp.sum(d_dist[:, None] * offset_vec, axis=3))
    return jnp.concatenate([direct, lax.optimization_barrier(jnp.sum(d_radius, axis=2))[:, None, :]], axis=1)

def chain_terms(side_i, side_j, mask):
    offset_vec, dist_sq = separation(side_i[:, 0:3], side_j[:, 0:3])
    value_ij, slope_ij = screening(dist_sq, side_i[:, 4][:, :, None], side_j[:, 4][:, None, :], side_j[:, 5][:, None, :], side_j[:, 6][:, None, :])
    value_ji, slope_ji = screening(dist_sq, side_j[:, 4][:, None, :], side_i[:, 4][:, :, None], side_i[:, 5][:, :, None], side_i[:, 6][:, :, None])
    factor = mask * (side_i[:, -1][:, :, None] * slope_ij + side_j[:, -1][:, None, :] * slope_ji)
    return -2.0 * lax.optimization_barrier(jnp.sum(factor[:, None] * offset_vec, axis=3))

def radius_terms(born_sum, intrinsic, coef_alpha, coef_beta, coef_gamma):
    scaled = intrinsic * born_sum
    poly_arg = coef_alpha * scaled - coef_beta * scaled * scaled + coef_gamma * scaled * scaled * scaled
    squash = jnp.tanh(poly_arg)
    radius = 1.0 / (1.0 / intrinsic - squash / (intrinsic + OFFSET))
    poly_slope = coef_alpha - 2.0 * coef_beta * scaled + 3.0 * coef_gamma * scaled * scaled
    radius_rate = radius * radius * (1.0 - squash * squash) * poly_slope * intrinsic / (intrinsic + OFFSET)
    return (radius, radius_rate)

def reference(positions, velocities, old_forces, charges, atom_types, type_table, tile_pairs):
    type_ids = jnp.arange(TYPES, dtype=jnp.int32)
    onehot = (atom_types[None, :] == type_ids[:, None]).astype(jnp.float32)
    params = lax.optimization_barrier(jnp.sum(type_table[:, :, None] * onehot[None, :, :], axis=1))
    atom_mass = params[6]
    new_positions = positions + TIMESTEP * velocities + TIMESTEP * TIMESTEP / (2.0 * atom_mass) * old_forces
    attrs = jnp.concatenate([new_positions, charges[None, :], params[0:6]], axis=0)
    block_count = ATOMS // TILE
    row_ids = jnp.arange(N_ROW, dtype=jnp.int32)[:, None, None]
    col_ids = jnp.arange(N_COL, dtype=jnp.int32)[None, :, None]
    live_slot = tile_pairs[:, :, 0, :] >= 0
    tiles_i = jnp.maximum(tile_pairs[:, :, 0, :], 0)
    tiles_j = jnp.maximum(tile_pairs[:, :, 1, :], 0)
    block_i = (row_ids * I_BLOCKS + tiles_i).astype(jnp.int32).reshape(-1, TILE_CAP)
    block_j = ((tiles_j // BLK_DEV * N_COL + col_ids) * BLK_DEV + tiles_j % BLK_DEV).astype(jnp.int32).reshape(-1, TILE_CAP)
    live_f = live_slot.astype(jnp.float32).reshape(-1, TILE_CAP)
    diagonal = jnp.eye(TILE, dtype=jnp.float32)

    def all_tiles(func, rows, packed):
        blocks = packed.reshape(packed.shape[0], block_count, TILE)

        def per_device(item):
            list_i, list_j, live_row = item
            side_i = jnp.moveaxis(jnp.take(blocks, list_i, axis=1), 1, 0)
            side_j = jnp.moveaxis(jnp.take(blocks, list_j, axis=1), 1, 0)
            self_pair = (list_i == list_j).astype(jnp.float32)
            mask = live_row[:, None, None] * (1.0 - self_pair[:, None, None] * diagonal)
            return func(side_i, side_j, mask)
        partial_sums = lax.map(per_device, (block_i, block_j, live_f))
        summed = jnp.zeros((block_count, rows, TILE), jnp.float32).at[block_i.reshape(-1)].add(partial_sums.reshape(-1, rows, TILE))
        return jnp.moveaxis(summed, 1, 0).reshape(rows, ATOMS)
    born_part = all_tiles(born_terms, 1, attrs)[0]
    radius, radius_rate = radius_terms(born_part, params[0], params[3], params[4], params[5])
    pair_part = all_tiles(pair_terms, 4, jnp.concatenate([attrs, radius[None, :]], axis=0))
    chain = (COULOMB * charges * charges / (2.0 * radius * radius) - COULOMB * pair_part[3]) * radius_rate
    chain_part = all_tiles(chain_terms, 3, jnp.concatenate([attrs, chain[None, :]], axis=0))
    new_forces = pair_part[0:3] + chain_part
    new_velocities = velocities + TIMESTEP / (2.0 * atom_mass) * (old_forces + new_forces)
    return (new_positions, new_velocities, new_forces)
```

```python
import functools
import math

import jax
import jax.numpy as jnp
from jax import lax
from jax.experimental import pallas as pl
from jax.experimental.pallas import tpu as pltpu
from jax.sharding import PartitionSpec as P

TILE = 128
STRIP = 8
CUTOFF_SQ = 144.0
COULOMB = 32.0
TIMESTEP = 0.5
OFFSET = 0.09
NECK_GAP = 0.5
NECK_WIDTH = 16.0
LOG2E = math.log2(math.e)
MESH = pl.DeviceIdType.MESH
SENT = 5
STRIPS = range(0, TILE, STRIP)
UNROLL_PEERS = 32


def kernel(
    rows, cols, blk_dev, table_in, tiles_in, pos_in, vel_in, frc_in, chg_in, typ_in,
    out,
    table_ref, tiles_ref, pos_ref, vel_ref, frc_ref, chg_ref, typ_ref, load_sem,
    own, recv, kinds, charge, side, total, radius, rate, chain_const, chain,
    turned, turned_rad, geo, mom, acc, early, part, partial_recv, grad_part, grad_recv, frc_part, frc_recv,
    send_sem, recv_sem,
):
    my_row, my_col = lax.axis_index("row"), lax.axis_index("col")
    devices = rows * cols
    blocks_j, blocks_i = rows * blk_dev, cols * blk_dev
    blocks = blocks_j + blocks_i
    base_i = total.shape[0] - -(-blocks_i // 8) * 8
    slots = tiles_ref.shape[1]
    types = table_ref.shape[1]

    def wrap(value, size):
        return jnp.where(value >= size, value - size, value)

    barrier = pltpu.get_barrier_semaphore()

    def each(first, last, action):
        if last - first <= UNROLL_PEERS:
            for step in range(first, last):
                action(step)
        else:
            def one(step, _):
                action(step)
                return 0

            lax.fori_loop(first, last, one, 0)

    def row_peer(step):
        return {"row": wrap(my_row + step, rows), "col": my_col}

    def col_peer(step):
        return {"row": my_row, "col": wrap(my_col + step, cols)}

    def greet(device):
        pl.semaphore_signal(barrier, inc=1, device_id=device, device_id_type=MESH)

    each(rows // 2, rows, lambda s: greet(row_peer(s)))
    each(1, rows // 2, lambda s: greet(row_peer(s)))
    each(1, cols, lambda s: greet(col_peer(s)))

    loads = [
        pltpu.make_async_copy(source, held, load_sem.at[k])
        for k, (source, held) in enumerate((
            (table_in, table_ref), (typ_in, typ_ref), (pos_in, pos_ref), (vel_in, vel_ref),
            (frc_in, frc_ref), (chg_in, chg_ref), (tiles_in.at[0, 0], tiles_ref),
        ))
    ]
    for load in loads:
        load.start()
    for load in loads:
        load.wait()

    mass = []
    for b in range(blk_dev):
        span = pl.ds(b * TILE, TILE)
        kind = typ_ref[b : b + 1, :].astype(jnp.float32)
        m = jnp.zeros((1, TILE), jnp.float32)
        for t in range(types):
            m = jnp.where(kind == t, table_ref[6, t], m)
        mass.append(m)
        held = []
        for k in range(3):
            x = (
                pos_ref[k : k + 1, span]
                + TIMESTEP * vel_ref[k : k + 1, span]
                + TIMESTEP * TIMESTEP / (2.0 * m) * frc_ref[k : k + 1, span]
            )
            out[0, k : k + 1, span] = x
            held.append(x)
        held += [chg_ref[b : b + 1, :], kind]
        for k, value in enumerate(held):
            own[k * blk_dev + b] = value
            recv[my_row, k * blk_dev + b] = value
            recv[rows + my_col, k * blk_dev + b] = value
    acc[...] = jnp.zeros_like(acc)
    kinds[...] = jnp.zeros_like(kinds)
    charge[...] = jnp.zeros_like(charge)
    total[...] = jnp.zeros_like(total)

    pl.semaphore_wait(barrier, rows + cols - 2)

    def copy0(slot, receive, device):
        pltpu.make_async_remote_copy(
            own, recv.at[slot], send_sem.at[0], recv_sem.at[receive],
            device_id=device, device_id_type=MESH,
        ).start()

    each(1, cols, lambda s: copy0(rows + my_col, 1, col_peer(s)))
    each(rows // 2, rows, lambda s: copy0(my_row, 0, row_peer(s)))
    each(1, rows // 2, lambda s: copy0(my_row, 0, row_peer(s)))

    def whole_of(ref, count, send, receive):
        piece = ref.at[pl.ds(0, count)]
        return pltpu.make_async_remote_copy(
            piece, piece, send_sem.at[send], recv_sem.at[receive],
            device_id={"row": my_row, "col": my_col}, device_id_type=MESH,
        )

    def by_type(kind, row):
        value = jnp.full(kind.shape, table_ref[row, 0], jnp.float32)
        for t in range(1, types):
            value = jnp.where(kind == t, table_ref[row, t], value)
        return value

    def wide(value):
        return jnp.broadcast_to(value, (STRIP, TILE))

    def turn(value, s=0):
        return pltpu.roll(wide(value), s, 1, stride=1, stride_axis=0)

    def back(value, s):
        return pltpu.roll(value, TILE - s, 1) if s else value

    def gather_up(value):
        level = value[0:1]
        for r in range(1, STRIP):
            level = level + back(value[r : r + 1], r)
        return level

    part_i, part_j = pl.ds(base_i, total.shape[0] - base_i), pl.ds(0, base_i)

    def spread_types(span):
        kind = kinds[span, :]
        rho = by_type(kind, 0)
        side[0, span, :] = rho
        side[1, span, :] = rho * rho
        side[2, span, :] = by_type(kind, 1) * rho * rho * rho * (1.0 / (CUTOFF_SQ * CUTOFF_SQ))
        side[3, span, :] = by_type(kind, 2) * (1.0 / (CUTOFF_SQ * CUTOFF_SQ))

    def unpack(held, k, slot, row):
        for b in range(blk_dev):
            held[pl.ds(row + b, 1), :] = recv[slot, k * blk_dev + b]

    whole_of(recv, cols - 1, 0, 1).wait_recv()
    for c in range(cols):
        unpack(kinds, 4, rows + c, base_i + c * blk_dev)
    spread_types(part_i)
    for a in range(blocks_i):
        c, b = a // blk_dev, a % blk_dev
        values = [recv[rows + c, k * blk_dev + b] for k in range(3)]
        row = slice(base_i + a, base_i + a + 1)
        values += [side[0, row, :], side[1, row, :], 2.0 * side[2, row, :], 2.0 * side[3, row, :]]
        for n, value in enumerate(values):
            for s in STRIPS:
                turned[n, a, s // STRIP] = turn(value, s)

    whole_of(recv, rows - 1, 0, 0).wait_recv()
    each(0, rows, lambda r: unpack(kinds, 4, r, r * blk_dev))
    spread_types(part_j)

    def tile_of(slot):
        first, second = tiles_ref[0, slot], tiles_ref[1, slot]
        return jnp.maximum(first, 0), jnp.maximum(second, 0), first

    def each_tile(sweep, first, want):
        group = max(g for g in range(1, want + 1) if slots % g == 0)

        def some(step, _):
            done = [sweep(step * group + k) for k in range(group)]
            for a in range(blocks_i):
                picks = [jnp.where(block == a, 1.0, 0.0) for block, _ in done]
                for n in range(len(done[0][1])):
                    level = acc[first + n, a]
                    for pick, (_, sums) in zip(picks, done):
                        level = level + pick * sums[n]
                    acc[first + n, a] = level
            return 0

        lax.fori_loop(0, slots // group, some, 0)

    def sent_row(k, block_j):
        return recv[lax.div(block_j, blk_dev), k * blk_dev + lax.rem(block_j, blk_dev)]

    def side_row(k, block_j):
        return wide(side[k, pl.ds(block_j, 1), :])

    def add(total_so_far, value):
        return value if total_so_far is None else total_so_far + value

    same_atom = jnp.where(lax.broadcasted_iota(jnp.int32, (STRIP, TILE), 0) == 0, CUTOFF_SQ, 0.0)

    def born_sweep(slot):
        bi, bj, first = tile_of(slot)
        live = jnp.where(first >= 0, CUTOFF_SQ, 0.0)
        global_i = my_row * blocks_i + bi
        global_j = (lax.div(bj, blk_dev) * cols + my_col) * blk_dev + lax.rem(bj, blk_dev)
        self_pair = jnp.where(global_i == global_j, 1.0, 0.0)
        xj, yj, zj = (wide(sent_row(k, bj)) for k in range(3))
        gap_j = side_row(0, bj) + NECK_GAP
        vol_j, neck_j = side_row(2, bj), side_row(3, bj)
        born = None
        for s in STRIPS:
            span = pl.ds(s, STRIP)
            xi, yi, zi, rho_i, rho_sq = (turned[k, bi, s // STRIP] for k in range(5))
            dx, dy, dz = xi - xj, yi - yj, zi - zj
            q = dx * dx + dy * dy + dz * dz
            t = jnp.maximum((live if s else live - self_pair * same_atom) - q, 0.0)
            t_sq = t * t
            inv = 1.0 / (q + rho_sq)
            gap = rho_i + gap_j
            off = q - gap * gap
            bump = jnp.exp2(off * off * (-LOG2E / NECK_WIDTH))
            born = add(born, back(t_sq * (vol_j * inv * inv + neck_j * bump), s))
            geo[0, slot, span, :] = q
            geo[1, slot, span, :] = t
            geo[2, slot, span, :] = t_sq
            geo[3, slot, span, :] = bump
        return bi, [born]

    each_tile(born_sweep, 0, 8)

    def exchange(index, scale, piece, landing, channel):
        for a in range(blocks_i):
            value = gather_up(acc[index, a]) * scale(a)
            piece[a] = value
            landing[my_col * blocks + blocks_j + a] = value
        for b in range(blk_dev):
            landing[my_col * blocks + my_row * blk_dev + b] = piece[my_col * blk_dev + b]

        def send(source, place, device):
            pltpu.make_async_remote_copy(
                source, landing.at[place], send_sem.at[channel], recv_sem.at[1 + channel],
                device_id=device, device_id_type=MESH,
            ).start()

        mine = pl.ds(my_col * blocks + my_row * blk_dev, blk_dev)
        for dc in reversed(range(cols)):
            peer_col = wrap(my_col + dc, cols)
            source = piece.at[pl.ds(peer_col * blk_dev, blk_dev)]

            def send_row(step):
                send(source, mine, {"row": wrap(my_row + step, rows), "col": peer_col})

            each(rows // 2, rows, send_row)
            each(0 if dc else 1, rows // 2, send_row)
        own_row = pl.ds(my_col * blocks + blocks_j, blocks_i)
        each(1, cols, lambda s: send(piece, own_row, col_peer(s)))
        count = (devices - 1) * blk_dev + (cols - 1) * blocks_i

        def finish():
            whole_of(landing, count, channel, 1 + channel).wait_recv()

            def summed(b):
                value = landing[b]
                for c in range(1, cols):
                    value = value + landing[c * blocks + b]
                row = b if b < blocks_j else b + base_i - blocks_j
                total[row : row + 1, :] = value

            for b in range(blocks):
                summed(b)

        def drain():
            whole_of(landing, count, channel, 1 + channel).wait_send()

        return finish, drain

    finish1, drain1 = exchange(0, lambda a: 1.0, part, partial_recv, 1)

    def slope_sweep(slot):
        bi, bj, _ = tile_of(slot)
        coords_j = [wide(sent_row(k, bj)) for k in range(3)]
        coords_i = [turned[k, bi, 0] for k in range(3)]
        gap_j = side_row(0, bj) + NECK_GAP
        rho_sq_j = side_row(1, bj)
        vol_j, neck_j = 2.0 * side_row(2, bj), 2.0 * side_row(3, bj)
        sums = [None] * 3
        for s in STRIPS:
            span = pl.ds(s, STRIP)
            rho_i, rho_sq, vol_i, neck_i = (turned[k, bi, s // STRIP] for k in range(3, 7))
            q, t, bump = geo[0, slot, span, :], geo[1, slot, span, :], geo[3, slot, span, :]
            soft_i, soft_j = q + rho_sq, q + rho_sq_j
            both = 1.0 / (soft_i * soft_j)
            inv_i, inv_j = both * soft_j, both * soft_i
            gap = rho_i + gap_j
            off = (q - gap * gap) * (1.0 / NECK_WIDTH)

            def slope(volume, neck, inv):
                far = volume * inv * inv
                near = neck * bump
                return t * (t * (far * inv + near * off) + (far + near))

            slope_ij = back(slope(vol_j, neck_j, inv_i), s)
            slope_ji = back(slope(vol_i, neck_i, inv_j), s)
            for k in range(3):
                d = coords_i[k] - back(coords_j[k], s)
                sums[k] = add(sums[k], slope_ij * d)
                geo[4 + k, slot, span, :] = d
                mom[k, slot, span, :] = slope_ji * d
        return bi, sums

    each_tile(slope_sweep, 1, 4)
    alpha, beta, gamma = (by_type(kinds[...], k) for k in (3, 4, 5))
    each(0, rows, lambda r: unpack(charge, 3, r, r * blk_dev))
    for c in range(cols):
        unpack(charge, 3, rows + c, base_i + c * blk_dev)
    for a in range(blocks_i):
        for k in range(3):
            early[k, a] = gather_up(acc[1 + k, a])
    finish1()

    rho = side[0]
    scaled = rho * total[...]
    squash = jnp.tanh(
        alpha * scaled - beta * scaled * scaled + gamma * scaled * scaled * scaled
    )
    rad = 1.0 / (1.0 / rho - squash / (rho + OFFSET))
    radius[0] = rad
    radius[1] = (-0.25 * LOG2E) / rad
    radius[2] = rad * charge[...]
    for a in range(blocks_i):
        for s in STRIPS:
            strip = turn(rad[base_i + a : base_i + a + 1, :], s)
            turned_rad[0, a, s // STRIP] = strip
            turned_rad[1, a, s // STRIP] = 1.0 / strip

    def pair_sweep(slot):
        bi, bj, _ = tile_of(slot)
        rad_j, over_j, rad_charge_j = (wide(radius[k, pl.ds(bj, 1), :]) for k in range(3))
        grad = None
        for s in STRIPS:
            span = pl.ds(s, STRIP)
            q, t_sq = geo[0, slot, span, :], geo[2, slot, span, :]
            power = q * (turned_rad[1, bi, s // STRIP] * over_j)
            decay = jnp.exp2(power)
            inv = lax.rsqrt(q + turned_rad[0, bi, s // STRIP] * rad_j * decay)
            lean = t_sq * (inv * inv * inv)
            grad = add(grad, back(lean * (decay * (LOG2E - power)) * rad_charge_j, s))
            geo[2, slot, span, :] = inv
            geo[3, slot, span, :] = decay
        return bi, [grad]

    each_tile(pair_sweep, 4, 8)
    grad_scale = -0.5 / (CUTOFF_SQ * CUTOFF_SQ * LOG2E)
    finish2, drain2 = exchange(
        4, lambda a: grad_scale * charge[base_i + a : base_i + a + 1, :], grad_part, grad_recv, 2
    )

    def direct_sweep(slot):
        bi, bj, _ = tile_of(slot)
        charge_j = wide(charge[pl.ds(bj, 1), :])
        sums = [None] * 3
        for s in STRIPS:
            span = pl.ds(s, STRIP)
            t, inv, decay = (geo[k, slot, span, :] for k in range(1, 4))
            steep = t * inv
            pull = back(steep * charge_j * (2.0 + steep * inv * (0.5 - 0.125 * decay)), s)
            for k in range(3):
                sums[k] = add(sums[k], pull * geo[4 + k, slot, span, :])
        return bi, sums

    each_tile(direct_sweep, 5, 4)
    scaled = rho * total[...]
    squash = jnp.tanh(
        alpha * scaled - beta * scaled * scaled + gamma * scaled * scaled * scaled
    )
    rad = radius[0]
    slow = (
        COULOMB * rad * rad * (1.0 - squash * squash)
        * (alpha - 2.0 * beta * scaled + 3.0 * gamma * scaled * scaled)
        * rho / (rho + OFFSET)
    )
    rate[...] = slow
    chain_const[...] = (0.5 * charge[...] * charge[...] / (rad * rad)) * slow
    direct_scale = -2.0 * COULOMB / (CUTOFF_SQ * CUTOFF_SQ)
    for a in range(blocks_i):
        for k in range(3):
            early[3 + k, a] = direct_scale * charge[base_i + a : base_i + a + 1, :] * gather_up(acc[5 + k, a])
    finish2()
    chain[...] = chain_const[...] - rate[...] * total[...]

    def chain_sweep(slot):
        bi, bj, _ = tile_of(slot)
        base = wide(chain[pl.ds(bj, 1), :])
        sums = [None] * 3
        for s in STRIPS:
            span = pl.ds(s, STRIP)
            factor = back(base, s)
            for k in range(3):
                sums[k] = add(sums[k], factor * mom[k, slot, span, :])
        return bi, sums

    each_tile(chain_sweep, 8, 8)

    for a in range(blocks_i):
        chain_i = chain[base_i + a : base_i + a + 1, :]
        for k in range(3):
            frc_part[a // blk_dev, k * blk_dev + a % blk_dev] = (
                early[3 + k, a] + 2.0 * (chain_i * early[k, a] + gather_up(acc[8 + k, a]))
            )

    for step in range(1, cols):
        peer_col = wrap(my_col + step, cols)
        pltpu.make_async_remote_copy(
            frc_part.at[peer_col], frc_recv.at[my_col], send_sem.at[3], recv_sem.at[4],
            device_id={"row": my_row, "col": peer_col}, device_id_type=MESH,
        ).start()
    frc_recv[my_col] = frc_part[my_col]
    whole_of(recv, rows + cols - 2, 0, 0).wait_send()
    drain1()
    drain2()
    whole_of(frc_recv, cols - 1, 3, 4).wait_recv()
    for b in range(blk_dev):
        span = pl.ds(b * TILE, TILE)
        for k in range(3):
            value = frc_recv[0, k * blk_dev + b]
            for c in range(1, cols):
                value = value + frc_recv[c, k * blk_dev + b]
            out[1, k : k + 1, span] = value
            out[2, k : k + 1, span] = vel_ref[k : k + 1, span] + TIMESTEP / (2.0 * mass[b]) * (
                frc_ref[k : k + 1, span] + value
            )
    whole_of(frc_part, cols - 1, 3, 4).wait_send()


def solution(mesh):
    rows, cols = mesh.shape["row"], mesh.shape["col"]

    def body(positions, velocities, old_forces, charges, atom_types, type_table, tile_pairs):
        blk_dev = positions.shape[1] // TILE
        slots = tile_pairs.shape[-1]
        blocks_i, blocks_j = cols * blk_dev, rows * blk_dev
        blocks = -(-blocks_i // 8) * 8 + -(-blocks_j // 8) * 8
        landed = cols * (blocks_i + blocks_j)
        vmem = pl.BlockSpec(memory_space=pltpu.VMEM)
        anywhere = pl.BlockSpec(memory_space=pl.ANY)
        f32 = lambda *shape: pltpu.VMEM(shape, jnp.float32)
        dma = lambda n: pltpu.SemaphoreType.DMA((n,))
        out = pl.pallas_call(
            functools.partial(kernel, rows, cols, blk_dev),
            out_shape=pltpu.VMEM((3,) + positions.shape, jnp.float32),
            in_specs=[anywhere] * 7,
            out_specs=vmem,
            scratch_shapes=[
                pltpu.SMEM(type_table.shape, jnp.float32),
                pltpu.SMEM(tile_pairs.shape[2:], jnp.int32),
                f32(*positions.shape), f32(*positions.shape), f32(*positions.shape),
                f32(blk_dev, TILE),
                pltpu.VMEM((blk_dev, TILE), jnp.int32),
                dma(7),
                f32(SENT * blk_dev, 1, TILE),
                f32(rows + cols, SENT * blk_dev, 1, TILE),
                f32(blocks, TILE),
                f32(blocks, TILE),
                f32(4, blocks, TILE),
                f32(blocks, TILE),
                f32(3, blocks, TILE),
                f32(blocks, TILE),
                f32(blocks, TILE),
                f32(blocks, TILE),
                f32(7, blocks_i, TILE // STRIP, STRIP, TILE),
                f32(2, blocks_i, TILE // STRIP, STRIP, TILE),
                f32(7, slots, TILE, TILE),
                f32(3, slots, TILE, TILE),
                f32(11, blocks_i, STRIP, TILE),
                f32(6, blocks_i, 1, TILE),
                f32(blocks_i, 1, TILE),
                f32(landed, 1, TILE),
                f32(blocks_i, 1, TILE),
                f32(landed, 1, TILE),
                f32(cols, 3 * blk_dev, 1, TILE),
                f32(cols, 3 * blk_dev, 1, TILE),
                dma(4), dma(5),
            ],
            compiler_params=pltpu.CompilerParams(
                collective_id=0, has_side_effects=True, vmem_limit_bytes=60000 * 1024
            ),
            name="verlet",
        )(
            type_table, tile_pairs, positions, velocities, old_forces,
            charges.reshape(blk_dev, TILE), atom_types.reshape(blk_dev, TILE),
        )
        return out[0], out[2], out[1]

    return jax.shard_map(
        body,
        mesh=mesh,
        in_specs=(
            P(None, ("row", "col")),
            P(None, ("row", "col")),
            P(None, ("row", "col")),
            P(("row", "col")),
            P(("row", "col")),
            P(),
            P("row", "col", None, None),
        ),
        out_specs=(P(None, ("row", "col")), P(None, ("row", "col")), P(None, ("row", "col"))),
        check_vma=False,
    )
```

```python
import functools
import math

import jax
import jax.numpy as jnp
from jax import lax
from jax.experimental import pallas as pl
from jax.experimental.pallas import tpu as pltpu
from jax.sharding import PartitionSpec as P

TILE = 128
STRIP = 8
CUTOFF_SQ = 144.0
COULOMB = 32.0
TIMESTEP = 0.5
OFFSET = 0.09
NECK_GAP = 0.5
NECK_WIDTH = 16.0
LOG2E = math.log2(math.e)
MESH = pl.DeviceIdType.MESH
SENT = 4
STRIPS = range(0, TILE, STRIP)
UNROLL_PEERS = 32
CUTOFF = 12.0
DENSITY = 0.1


def near_rows(rows, row_blocks):
    side = round((rows * row_blocks) ** (1.0 / 3.0))
    side += side ** 3 < rows * row_blocks
    plane = side * side
    reach = int(CUTOFF / (TILE / DENSITY) ** (1.0 / 3.0)) + 1

    def interval(r):
        low = (r * row_blocks) // plane - reach
        high = ((r + 1) * row_blocks - 1) // plane + reach
        first = (jnp.maximum(low, 0) * plane) // row_blocks
        last = jnp.minimum(((high + 1) * plane - 1) // row_blocks, rows - 1)
        return first, last - first + 1

    with jax.ensure_compile_time_eval():
        counts = sorted({int(interval(r)[1]) for r in range(rows)})
    return interval, counts


def kernel(
    rows, cols, blk_dev, table_in, tiles_in, pos_in, vel_in, frc_in, chg_in, typ_in,
    out,
    table_ref, tiles_ref, pos_ref, vel_ref, frc_ref, chg_ref, typ_ref, load_sem,
    own, recv, own_charge, recv_charge, kinds, charge, side, total, radius, rate, chain_const, chain,
    turned, turned_rad, geo, mom, acc, early, part, partial_recv, grad_part, grad_recv, frc_part, frc_recv,
    send_sem, recv_sem,
):
    my_row, my_col = lax.axis_index("row"), lax.axis_index("col")
    blocks_j, blocks_i = rows * blk_dev, cols * blk_dev
    blocks = blocks_j + blocks_i
    base_i = total.shape[0] - -(-blocks_i // 8) * 8
    slots = tiles_ref.shape[1]
    types = table_ref.shape[1]

    def wrap(value, size):
        return jnp.where(value >= size, value - size, value)

    loads = [
        pltpu.make_async_copy(source, held, load_sem.at[k])
        for k, (source, held) in enumerate((
            (table_in, table_ref), (typ_in, typ_ref), (pos_in, pos_ref), (vel_in, vel_ref),
            (frc_in, frc_ref), (chg_in, chg_ref), (tiles_in.at[0, 0], tiles_ref),
        ))
    ]
    for load in loads:
        load.start()

    barrier = pltpu.get_barrier_semaphore()

    def each(first, last, action):
        if last - first <= UNROLL_PEERS:
            for step in range(first, last):
                action(step)
        else:
            def one(step, _):
                action(step)
                return 0

            lax.fori_loop(first, last, one, 0)

    interval, counts = near_rows(rows, blocks_i)
    first_row, row_count = interval(my_row)

    def by_count(action):
        if len(counts) == 1:
            action(counts[0])
        else:
            for n in counts:
                pl.when(row_count == n)(functools.partial(action, n))

    def each_row(n, first, action):
        part = max(rows // 4, 1)

        def at(step):
            action(first_row + wrap(my_row - first_row + step, n))

        each(min(2 * part, n), min(3 * part, n), at)
        each(min(part, n), min(2 * part, n), at)
        each(min(3 * part, n), n, at)
        each(first, min(part, n), at)

    def row_peer(peer_row):
        return {"row": peer_row, "col": my_col}

    def col_peer(step):
        return {"row": my_row, "col": wrap(my_col + step, cols)}

    def greet(device):
        pl.semaphore_signal(barrier, inc=1, device_id=device, device_id_type=MESH)

    by_count(lambda n: each_row(n, 1, lambda r: greet(row_peer(r))))
    each(1, cols, lambda s: greet(col_peer(s)))

    def clear_far(n):
        def clear(step):
            far = wrap(first_row + n + step, rows)
            recv[far] = jnp.zeros_like(recv[0])
            recv_charge[far] = jnp.zeros_like(recv_charge[0])
            for c in range(cols):
                for b in range(blk_dev):
                    place = c * blocks + far * blk_dev + b
                    partial_recv[place] = jnp.zeros((1, TILE), jnp.float32)
                    grad_recv[place] = jnp.zeros((1, TILE), jnp.float32)

        each(0, rows - n, clear)

    by_count(clear_far)

    for load in loads:
        load.wait()

    mass = []
    for b in range(blk_dev):
        span = pl.ds(b * TILE, TILE)
        kind = typ_ref[b : b + 1, :].astype(jnp.float32)
        m = jnp.zeros((1, TILE), jnp.float32)
        for t in range(types):
            m = jnp.where(kind == t, table_ref[6, t], m)
        mass.append(m)
        held = []
        for k in range(3):
            x = (
                pos_ref[k : k + 1, span]
                + TIMESTEP * vel_ref[k : k + 1, span]
                + TIMESTEP * TIMESTEP / (2.0 * m) * frc_ref[k : k + 1, span]
            )
            out[0, k : k + 1, span] = x
            held.append(x)
        for k, value in enumerate(held + [kind]):
            own[k * blk_dev + b] = value
            recv[my_row, k * blk_dev + b] = value
            recv[rows + my_col, k * blk_dev + b] = value
        value = chg_ref[b : b + 1, :]
        own_charge[b] = value
        recv_charge[my_row, b] = value
        recv_charge[rows + my_col, b] = value
    acc[...] = jnp.zeros_like(acc)
    kinds[...] = jnp.zeros_like(kinds)
    charge[...] = jnp.zeros_like(charge)
    total[...] = jnp.zeros_like(total)

    pl.semaphore_wait(barrier, row_count + cols - 2)

    def copy0(source, held, slot, send, receive, device):
        pltpu.make_async_remote_copy(
            source, held.at[slot], send_sem.at[send], recv_sem.at[receive],
            device_id=device, device_id_type=MESH,
        ).start()

    def copy0_rows(source, held, send, receive):
        by_count(lambda n: each_row(n, 1, lambda r: copy0(source, held, my_row, send, receive, row_peer(r))))

    def copy0_cols(source, held, send, receive):
        each(1, cols, lambda s: copy0(source, held, rows + my_col, send, receive, col_peer(s)))

    copy0_rows(own, recv, 0, 0)
    copy0_cols(own, recv, 0, 1)
    copy0_rows(own_charge, recv_charge, 4, 5)
    copy0_cols(own_charge, recv_charge, 4, 5)

    def whole_of(ref, count, send, receive):
        piece = ref.at[pl.ds(0, count)]
        return pltpu.make_async_remote_copy(
            piece, piece, send_sem.at[send], recv_sem.at[receive],
            device_id={"row": my_row, "col": my_col}, device_id_type=MESH,
        )

    def by_type(kind, row):
        value = jnp.full(kind.shape, table_ref[row, 0], jnp.float32)
        for t in range(1, types):
            value = jnp.where(kind == t, table_ref[row, t], value)
        return value

    def wide(value):
        return jnp.broadcast_to(value, (STRIP, TILE))

    def turn(value, s=0):
        return pltpu.roll(wide(value), s, 1, stride=1, stride_axis=0)

    def add(total_so_far, value):
        return value if total_so_far is None else total_so_far + value

    def back(value, s):
        return pltpu.roll(value, TILE - s, 1) if s else value

    def gather_up(first, count=1):
        held, level = count * blocks_i, None
        for r in range(STRIP):
            rows_r = acc[pl.ds(first * blocks_i * STRIP + r, held, stride=STRIP), :]
            level = add(level, back(rows_r, r))
        return level

    part_i, part_j = pl.ds(base_i, total.shape[0] - base_i), pl.ds(0, base_i)

    def spread_types(span):
        kind = kinds[span, :]
        rho = by_type(kind, 0)
        side[0, span, :] = rho
        side[1, span, :] = rho * rho
        side[2, span, :] = by_type(kind, 1) * rho * rho * rho * (1.0 / (CUTOFF_SQ * CUTOFF_SQ))
        side[3, span, :] = by_type(kind, 2) * (1.0 / (CUTOFF_SQ * CUTOFF_SQ))

    def unpack(held, source, first, slot, row):
        for b in range(blk_dev):
            held[pl.ds(row + b, 1), :] = source[slot, first + b]

    whole_of(recv, cols - 1, 0, 1).wait_recv()
    for c in range(cols):
        unpack(kinds, recv, 3 * blk_dev, rows + c, base_i + c * blk_dev)
    spread_types(part_i)
    for a in range(blocks_i):
        c, b = a // blk_dev, a % blk_dev
        values = [recv[rows + c, k * blk_dev + b] for k in range(3)]
        row = slice(base_i + a, base_i + a + 1)
        values += [side[0, row, :], side[1, row, :], 2.0 * side[2, row, :], 2.0 * side[3, row, :]]
        for n, value in enumerate(values):
            for s in STRIPS:
                turned[n, a, s // STRIP] = turn(value, s)

    by_count(lambda n: whole_of(recv, n - 1, 0, 0).wait_recv())
    each(0, rows, lambda r: unpack(kinds, recv, 3 * blk_dev, r, r * blk_dev))
    spread_types(part_j)

    def tile_of(slot):
        first, second = tiles_ref[0, slot], tiles_ref[1, slot]
        return jnp.maximum(first, 0), jnp.maximum(second, 0), first

    def each_tile(sweep, first, want):
        most = min(want, max(64 // blocks_i, 1))
        group = max(g for g in range(1, most + 1) if slots % g == 0)

        def some(step, _):
            done = [sweep(step * group + k) for k in range(group)]
            for a in range(blocks_i):
                picks = [jnp.where(block == a, 1.0, 0.0) for block, _ in done]
                for n in range(len(done[0][1])):
                    place = pl.ds(((first + n) * blocks_i + a) * STRIP, STRIP)
                    level = acc[place, :]
                    for pick, (_, sums) in zip(picks, done):
                        level = level + pick * sums[n]
                    acc[place, :] = level
            return 0

        lax.fori_loop(0, slots // group, some, 0)

    def sent_row(k, block_j):
        return recv[lax.div(block_j, blk_dev), k * blk_dev + lax.rem(block_j, blk_dev)]

    def side_row(k, block_j):
        return wide(side[k, pl.ds(block_j, 1), :])

    same_atom = jnp.where(lax.broadcasted_iota(jnp.int32, (STRIP, TILE), 0) == 0, CUTOFF_SQ, 0.0)

    def born_sweep(slot):
        bi, bj, first = tile_of(slot)
        live = jnp.where(first >= 0, CUTOFF_SQ, 0.0)
        global_i = my_row * blocks_i + bi
        global_j = (lax.div(bj, blk_dev) * cols + my_col) * blk_dev + lax.rem(bj, blk_dev)
        self_pair = jnp.where(global_i == global_j, 1.0, 0.0)
        xj, yj, zj = (wide(sent_row(k, bj)) for k in range(3))
        gap_j = side_row(0, bj) + NECK_GAP
        vol_j, neck_j = side_row(2, bj), side_row(3, bj)
        born = None
        for s in STRIPS:
            span = pl.ds(s, STRIP)
            xi, yi, zi, rho_i, rho_sq = (turned[k, bi, s // STRIP] for k in range(5))
            dx, dy, dz = xi - xj, yi - yj, zi - zj
            q = dx * dx + dy * dy + dz * dz
            t = jnp.maximum((live if s else live - self_pair * same_atom) - q, 0.0)
            t_sq = t * t
            inv = 1.0 / (q + rho_sq)
            gap = rho_i + gap_j
            off = q - gap * gap
            bump = jnp.exp2(off * off * (-LOG2E / NECK_WIDTH))
            born = add(born, back(t_sq * (vol_j * inv * inv + neck_j * bump), s))
            geo[0, slot, span, :] = q
            geo[1, slot, span, :] = t
            geo[2, slot, span, :] = t_sq
            geo[3, slot, span, :] = bump
        return bi, [born]

    each_tile(born_sweep, 0, 16)

    def exchange(index, scale, piece, landing, channel):
        gathered = gather_up(index)
        for a in range(blocks_i):
            value = gathered[a : a + 1, :] * scale(a)
            piece[a] = value
            landing[my_col * blocks + blocks_j + a] = value
        for b in range(blk_dev):
            landing[my_col * blocks + my_row * blk_dev + b] = piece[my_col * blk_dev + b]

        def send(source, place, device):
            pltpu.make_async_remote_copy(
                source, landing.at[place], send_sem.at[channel], recv_sem.at[1 + channel],
                device_id=device, device_id_type=MESH,
            ).start()

        mine = pl.ds(my_col * blocks + my_row * blk_dev, blk_dev)

        def send_all(n):
            for dc in reversed(range(cols)):
                peer_col = wrap(my_col + dc, cols)
                source = piece.at[pl.ds(peer_col * blk_dev, blk_dev)]
                each_row(n, 0 if dc else 1, lambda r: send(source, mine, {"row": r, "col": peer_col}))

        by_count(send_all)
        own_row = pl.ds(my_col * blocks + blocks_j, blocks_i)
        each(1, cols, lambda s: send(piece, own_row, col_peer(s)))

        def all_of(n):
            return whole_of(landing, (n * cols - 1) * blk_dev + (cols - 1) * blocks_i, channel, 1 + channel)

        def finish():
            by_count(lambda n: all_of(n).wait_recv())

            def summed(b):
                value = landing[b]
                for c in range(1, cols):
                    value = value + landing[c * blocks + b]
                row = b if b < blocks_j else b + base_i - blocks_j
                total[row : row + 1, :] = value

            for b in range(blocks):
                summed(b)

        def drain():
            by_count(lambda n: all_of(n).wait_send())

        return finish, drain

    finish1, drain1 = exchange(0, lambda a: 1.0, part, partial_recv, 1)

    def slope_sweep(slot):
        bi, bj, _ = tile_of(slot)
        coords_j = [wide(sent_row(k, bj)) for k in range(3)]
        coords_i = [turned[k, bi, 0] for k in range(3)]
        gap_j = side_row(0, bj) + NECK_GAP
        rho_sq_j = side_row(1, bj)
        vol_j, neck_j = 2.0 * side_row(2, bj), 2.0 * side_row(3, bj)
        sums = [None] * 3
        for s in STRIPS:
            span = pl.ds(s, STRIP)
            rho_i, rho_sq, vol_i, neck_i = (turned[k, bi, s // STRIP] for k in range(3, 7))
            q, t, bump = geo[0, slot, span, :], geo[1, slot, span, :], geo[3, slot, span, :]
            soft_i, soft_j = q + rho_sq, q + rho_sq_j
            both = 1.0 / (soft_i * soft_j)
            inv_i, inv_j = both * soft_j, both * soft_i
            gap = rho_i + gap_j
            off = (q - gap * gap) * (1.0 / NECK_WIDTH)

            def slope(volume, neck, inv):
                far = volume * inv * inv
                near = neck * bump
                return t * (t * (far * inv + near * off) + (far + near))

            slope_ij = back(slope(vol_j, neck_j, inv_i), s)
            slope_ji = back(slope(vol_i, neck_i, inv_j), s)
            for k in range(3):
                d = coords_i[k] - back(coords_j[k], s)
                sums[k] = add(sums[k], slope_ij * d)
                geo[4 + k, slot, span, :] = d
                mom[k, slot, span, :] = slope_ji * d
        return bi, sums

    each_tile(slope_sweep, 1, 4)
    alpha, beta, gamma = (by_type(kinds[...], k) for k in (3, 4, 5))
    by_count(lambda n: whole_of(recv_charge, n + cols - 2, 0, 5).wait_recv())
    each(0, rows, lambda r: unpack(charge, recv_charge, 0, r, r * blk_dev))
    for c in range(cols):
        unpack(charge, recv_charge, 0, rows + c, base_i + c * blk_dev)
    early[0] = gather_up(1, 3)
    finish1()

    rho = side[0]
    scaled = rho * total[...]
    squash = jnp.tanh(
        alpha * scaled - beta * scaled * scaled + gamma * scaled * scaled * scaled
    )
    rad = 1.0 / (1.0 / rho - squash / (rho + OFFSET))
    radius[0] = rad
    radius[1] = (-0.25 * LOG2E) / rad
    radius[2] = rad * charge[...]
    for a in range(blocks_i):
        for s in STRIPS:
            strip = turn(rad[base_i + a : base_i + a + 1, :], s)
            turned_rad[0, a, s // STRIP] = strip
            turned_rad[1, a, s // STRIP] = 1.0 / strip

    def pair_sweep(slot):
        bi, bj, _ = tile_of(slot)
        rad_j, over_j, rad_charge_j = (wide(radius[k, pl.ds(bj, 1), :]) for k in range(3))
        grad = None
        for s in STRIPS:
            span = pl.ds(s, STRIP)
            q, t_sq = geo[0, slot, span, :], geo[2, slot, span, :]
            power = q * (turned_rad[1, bi, s // STRIP] * over_j)
            decay = jnp.exp2(power)
            inv = lax.rsqrt(q + turned_rad[0, bi, s // STRIP] * rad_j * decay)
            lean = t_sq * (inv * inv * inv)
            grad = add(grad, back(lean * (decay * (LOG2E - power)) * rad_charge_j, s))
            geo[2, slot, span, :] = inv
            geo[3, slot, span, :] = decay
        return bi, [grad]

    each_tile(pair_sweep, 4, 16)
    grad_scale = -0.5 / (CUTOFF_SQ * CUTOFF_SQ * LOG2E)
    finish2, drain2 = exchange(
        4, lambda a: grad_scale * charge[base_i + a : base_i + a + 1, :], grad_part, grad_recv, 2
    )

    def direct_sweep(slot):
        bi, bj, _ = tile_of(slot)
        charge_j = wide(charge[pl.ds(bj, 1), :])
        sums = [None] * 3
        for s in STRIPS:
            span = pl.ds(s, STRIP)
            t, inv, decay = (geo[k, slot, span, :] for k in range(1, 4))
            steep = t * inv
            pull = back(steep * charge_j * (2.0 + steep * inv * (0.5 - 0.125 * decay)), s)
            for k in range(3):
                sums[k] = add(sums[k], pull * geo[4 + k, slot, span, :])
        return bi, sums

    each_tile(direct_sweep, 5, 4)
    scaled = rho * total[...]
    squash = jnp.tanh(
        alpha * scaled - beta * scaled * scaled + gamma * scaled * scaled * scaled
    )
    rad = radius[0]
    slow = (
        COULOMB * rad * rad * (1.0 - squash * squash)
        * (alpha - 2.0 * beta * scaled + 3.0 * gamma * scaled * scaled)
        * rho / (rho + OFFSET)
    )
    rate[...] = slow
    chain_const[...] = (0.5 * charge[...] * charge[...] / (rad * rad)) * slow
    direct_scale = -2.0 * COULOMB / (CUTOFF_SQ * CUTOFF_SQ)
    gathered = gather_up(5, 3)
    charges_i = direct_scale * charge[base_i : base_i + blocks_i, :]
    early[1] = jnp.concatenate([charges_i] * 3, axis=0) * gathered
    finish2()
    chain[...] = chain_const[...] - rate[...] * total[...]

    def chain_sweep(slot):
        bi, bj, _ = tile_of(slot)
        base = wide(chain[pl.ds(bj, 1), :])
        sums = [None] * 3
        for s in STRIPS:
            span = pl.ds(s, STRIP)
            factor = back(base, s)
            for k in range(3):
                sums[k] = add(sums[k], factor * mom[k, slot, span, :])
        return bi, sums

    each_tile(chain_sweep, 8, 16)

    chain_i = jnp.concatenate([2.0 * chain[base_i : base_i + blocks_i, :]] * 3, axis=0)
    force = early[1] + chain_i * early[0] + 2.0 * gather_up(8, 3)
    for a in range(blocks_i):
        for k in range(3):
            row = k * blocks_i + a
            frc_part[a // blk_dev, k * blk_dev + a % blk_dev] = force[row : row + 1, :]

    for step in range(1, cols):
        peer_col = wrap(my_col + step, cols)
        pltpu.make_async_remote_copy(
            frc_part.at[peer_col], frc_recv.at[my_col], send_sem.at[3], recv_sem.at[4],
            device_id={"row": my_row, "col": peer_col}, device_id_type=MESH,
        ).start()
    frc_recv[my_col] = frc_part[my_col]
    by_count(lambda n: whole_of(recv, n + cols - 2, 0, 0).wait_send())
    by_count(lambda n: whole_of(recv_charge, n + cols - 2, 4, 5).wait_send())
    drain1()
    drain2()
    whole_of(frc_recv, cols - 1, 3, 4).wait_recv()
    for b in range(blk_dev):
        span = pl.ds(b * TILE, TILE)
        for k in range(3):
            value = frc_recv[0, k * blk_dev + b]
            for c in range(1, cols):
                value = value + frc_recv[c, k * blk_dev + b]
            out[1, k : k + 1, span] = value
            out[2, k : k + 1, span] = vel_ref[k : k + 1, span] + TIMESTEP / (2.0 * mass[b]) * (
                frc_ref[k : k + 1, span] + value
            )
    whole_of(frc_part, cols - 1, 3, 4).wait_send()


def solution(mesh):
    rows, cols = mesh.shape["row"], mesh.shape["col"]

    def body(positions, velocities, old_forces, charges, atom_types, type_table, tile_pairs):
        blk_dev = positions.shape[1] // TILE
        slots = tile_pairs.shape[-1]
        blocks_i, blocks_j = cols * blk_dev, rows * blk_dev
        blocks = -(-blocks_i // 8) * 8 + -(-blocks_j // 8) * 8
        landed = cols * (blocks_i + blocks_j)
        vmem = pl.BlockSpec(memory_space=pltpu.VMEM)
        anywhere = pl.BlockSpec(memory_space=pl.ANY)
        f32 = lambda *shape: pltpu.VMEM(shape, jnp.float32)
        dma = lambda n: pltpu.SemaphoreType.DMA((n,))
        out = pl.pallas_call(
            functools.partial(kernel, rows, cols, blk_dev),
            out_shape=pltpu.VMEM((3,) + positions.shape, jnp.float32),
            in_specs=[anywhere] * 7,
            out_specs=vmem,
            scratch_shapes=[
                pltpu.SMEM(type_table.shape, jnp.float32),
                pltpu.SMEM(tile_pairs.shape[2:], jnp.int32),
                f32(*positions.shape), f32(*positions.shape), f32(*positions.shape),
                f32(blk_dev, TILE),
                pltpu.VMEM((blk_dev, TILE), jnp.int32),
                dma(7),
                f32(SENT * blk_dev, 1, TILE),
                f32(rows + cols, SENT * blk_dev, 1, TILE),
                f32(blk_dev, 1, TILE),
                f32(rows + cols, blk_dev, 1, TILE),
                f32(blocks, TILE),
                f32(blocks, TILE),
                f32(4, blocks, TILE),
                f32(blocks, TILE),
                f32(3, blocks, TILE),
                f32(blocks, TILE),
                f32(blocks, TILE),
                f32(blocks, TILE),
                f32(7, blocks_i, TILE // STRIP, STRIP, TILE),
                f32(2, blocks_i, TILE // STRIP, STRIP, TILE),
                f32(7, slots, TILE, TILE),
                f32(3, slots, TILE, TILE),
                f32(11 * blocks_i * STRIP, TILE),
                f32(2, 3 * blocks_i, TILE),
                f32(blocks_i, 1, TILE),
                f32(landed, 1, TILE),
                f32(blocks_i, 1, TILE),
                f32(landed, 1, TILE),
                f32(cols, 3 * blk_dev, 1, TILE),
                f32(cols, 3 * blk_dev, 1, TILE),
                dma(5), dma(6),
            ],
            compiler_params=pltpu.CompilerParams(
                collective_id=0, has_side_effects=True, vmem_limit_bytes=60000 * 1024
            ),
            name="verlet",
        )(
            type_table, tile_pairs, positions, velocities, old_forces,
            charges.reshape(blk_dev, TILE), atom_types.reshape(blk_dev, TILE),
        )
        return out[0], out[2], out[1]

    return jax.shard_map(
        body,
        mesh=mesh,
        in_specs=(
            P(None, ("row", "col")),
            P(None, ("row", "col")),
            P(None, ("row", "col")),
            P(("row", "col")),
            P(("row", "col")),
            P(),
            P("row", "col", None, None),
        ),
        out_specs=(P(None, ("row", "col")), P(None, ("row", "col")), P(None, ("row", "col"))),
        check_vma=False,
    )
```

```python
import functools
import math

import jax
import jax.numpy as jnp
from jax import lax
from jax.experimental import pallas as pl
from jax.experimental.pallas import tpu as pltpu
from jax.sharding import PartitionSpec as P

TILE = 128
STRIP = 8
CUTOFF_SQ = 144.0
COULOMB = 32.0
TIMESTEP = 0.5
OFFSET = 0.09
NECK_GAP = 0.5
NECK_WIDTH = 16.0
LOG2E = math.log2(math.e)
MESH = pl.DeviceIdType.MESH
SENT = 4
STRIPS = range(0, TILE, STRIP)
UNROLL_PEERS = 32
EARLY_SLOPES = 24
CUTOFF = 12.0
DENSITY = 0.1


def near_rows(rows, row_blocks):
    side = round((rows * row_blocks) ** (1.0 / 3.0))
    side += side ** 3 < rows * row_blocks
    plane = side * side
    reach = int(CUTOFF / (TILE / DENSITY) ** (1.0 / 3.0)) + 1

    def interval(r):
        low = (r * row_blocks) // plane - reach
        high = ((r + 1) * row_blocks - 1) // plane + reach
        first = (jnp.maximum(low, 0) * plane) // row_blocks
        last = jnp.minimum(((high + 1) * plane - 1) // row_blocks, rows - 1)
        return first, last - first + 1

    with jax.ensure_compile_time_eval():
        counts = sorted({int(interval(r)[1]) for r in range(rows)})
    return interval, counts


def kernel(
    rows, cols, blk_dev, table_in, tiles_in, pos_in, vel_in, frc_in, chg_in, typ_in,
    out,
    table_ref, tiles_ref, pos_ref, vel_ref, frc_ref, chg_ref, typ_ref, load_sem,
    own, recv, own_charge, recv_charge, kinds, charge, side, total, radius, rate, chain_const, chain,
    turned, turned_rad, geo, mom, acc, early, part, partial_recv, grad_part, grad_recv, frc_part, frc_recv,
    send_sem, recv_sem,
):
    my_row, my_col = lax.axis_index("row"), lax.axis_index("col")
    blocks_j, blocks_i = rows * blk_dev, cols * blk_dev
    blocks = blocks_j + blocks_i
    base_i = total.shape[0] - -(-blocks_i // 8) * 8
    slots = tiles_ref.shape[1]
    types = table_ref.shape[1]

    def wrap(value, size):
        return jnp.where(value >= size, value - size, value)

    loads = [
        pltpu.make_async_copy(source, held, load_sem.at[k])
        for k, (source, held) in enumerate((
            (table_in, table_ref), (typ_in, typ_ref), (pos_in, pos_ref), (vel_in, vel_ref),
            (frc_in, frc_ref), (chg_in, chg_ref), (tiles_in.at[0, 0], tiles_ref),
        ))
    ]
    for load in loads:
        load.start()

    barrier = pltpu.get_barrier_semaphore()

    def each(first, last, action):
        if last - first <= UNROLL_PEERS:
            for step in range(first, last):
                action(step)
        else:
            def one(step, _):
                action(step)
                return 0

            lax.fori_loop(first, last, one, 0)

    interval, counts = near_rows(rows, blocks_i)
    first_row, row_count = interval(my_row)

    def by_count(action):
        if len(counts) == 1:
            action(counts[0])
        else:
            for n in counts:
                pl.when(row_count == n)(functools.partial(action, n))

    def each_row(n, first, action):
        part = max(rows // 4, 1)

        def at(step):
            action(first_row + wrap(my_row - first_row + step, n))

        each(min(2 * part, n), min(3 * part, n), at)
        each(min(part, n), min(2 * part, n), at)
        each(min(3 * part, n), n, at)
        each(first, min(part, n), at)

    def row_peer(peer_row):
        return {"row": peer_row, "col": my_col}

    def col_peer(step):
        return {"row": my_row, "col": wrap(my_col + step, cols)}

    def greet(device):
        pl.semaphore_signal(barrier, inc=1, device_id=device, device_id_type=MESH)

    by_count(lambda n: each_row(n, 1, lambda r: greet(row_peer(r))))
    each(1, cols, lambda s: greet(col_peer(s)))

    def clear_far(n):
        def clear(step):
            far = wrap(first_row + n + step, rows)
            recv[far] = jnp.zeros_like(recv[0])
            recv_charge[far] = jnp.zeros_like(recv_charge[0])
            for c in range(cols):
                for b in range(blk_dev):
                    place = c * blocks + far * blk_dev + b
                    partial_recv[place] = jnp.zeros((1, TILE), jnp.float32)
                    grad_recv[place] = jnp.zeros((1, TILE), jnp.float32)

        each(0, rows - n, clear)

    by_count(clear_far)

    for load in loads:
        load.wait()

    mass = []
    for b in range(blk_dev):
        span = pl.ds(b * TILE, TILE)
        kind = typ_ref[b : b + 1, :].astype(jnp.float32)
        m = jnp.zeros((1, TILE), jnp.float32)
        for t in range(types):
            m = jnp.where(kind == t, table_ref[6, t], m)
        mass.append(m)
        held = []
        for k in range(3):
            x = (
                pos_ref[k : k + 1, span]
                + TIMESTEP * vel_ref[k : k + 1, span]
                + TIMESTEP * TIMESTEP / (2.0 * m) * frc_ref[k : k + 1, span]
            )
            out[0, k : k + 1, span] = x
            held.append(x)
        for k, value in enumerate(held + [kind]):
            own[k * blk_dev + b] = value
            recv[my_row, k * blk_dev + b] = value
            recv[rows + my_col, k * blk_dev + b] = value
        value = chg_ref[b : b + 1, :]
        own_charge[b] = value
        recv_charge[my_row, b] = value
        recv_charge[rows + my_col, b] = value
    acc[...] = jnp.zeros_like(acc)
    kinds[...] = jnp.zeros_like(kinds)
    charge[...] = jnp.zeros_like(charge)
    total[...] = jnp.zeros_like(total)

    pl.semaphore_wait(barrier, row_count + cols - 2)

    def copy0(source, held, slot, send, receive, device):
        pltpu.make_async_remote_copy(
            source, held.at[slot], send_sem.at[send], recv_sem.at[receive],
            device_id=device, device_id_type=MESH,
        ).start()

    def copy0_rows(source, held, send, receive):
        by_count(lambda n: each_row(n, 1, lambda r: copy0(source, held, my_row, send, receive, row_peer(r))))

    def copy0_cols(source, held, send, receive):
        each(1, cols, lambda s: copy0(source, held, rows + my_col, send, receive, col_peer(s)))

    copy0_rows(own, recv, 0, 0)
    copy0_cols(own, recv, 0, 1)
    copy0_rows(own_charge, recv_charge, 4, 5)
    copy0_cols(own_charge, recv_charge, 4, 5)

    def whole_of(ref, count, send, receive):
        piece = ref.at[pl.ds(0, count)]
        return pltpu.make_async_remote_copy(
            piece, piece, send_sem.at[send], recv_sem.at[receive],
            device_id={"row": my_row, "col": my_col}, device_id_type=MESH,
        )

    def by_type(kind, row):
        value = jnp.full(kind.shape, table_ref[row, 0], jnp.float32)
        for t in range(1, types):
            value = jnp.where(kind == t, table_ref[row, t], value)
        return value

    def wide(value):
        return jnp.broadcast_to(value, (STRIP, TILE))

    def turn(value, s=0):
        return pltpu.roll(wide(value), s, 1, stride=1, stride_axis=0)

    def add(total_so_far, value):
        return value if total_so_far is None else total_so_far + value

    def back(value, s):
        return pltpu.roll(value, TILE - s, 1) if s else value

    def gather_up(first, count=1):
        held, level = count * blocks_i, None
        for r in range(STRIP):
            rows_r = acc[pl.ds(first * blocks_i * STRIP + r, held, stride=STRIP), :]
            level = add(level, back(rows_r, r))
        return level

    part_i, part_j = pl.ds(base_i, total.shape[0] - base_i), pl.ds(0, base_i)

    def spread_types(span):
        kind = kinds[span, :]
        rho = by_type(kind, 0)
        side[0, span, :] = rho
        side[1, span, :] = rho * rho
        side[2, span, :] = by_type(kind, 1) * rho * rho * rho * (1.0 / (CUTOFF_SQ * CUTOFF_SQ))
        side[3, span, :] = by_type(kind, 2) * (1.0 / (CUTOFF_SQ * CUTOFF_SQ))

    def unpack(held, source, first, slot, row):
        for b in range(blk_dev):
            held[pl.ds(row + b, 1), :] = source[slot, first + b]

    whole_of(recv, cols - 1, 0, 1).wait_recv()
    for c in range(cols):
        unpack(kinds, recv, 3 * blk_dev, rows + c, base_i + c * blk_dev)
    spread_types(part_i)
    for a in range(blocks_i):
        c, b = a // blk_dev, a % blk_dev
        values = [recv[rows + c, k * blk_dev + b] for k in range(3)]
        row = slice(base_i + a, base_i + a + 1)
        values += [side[0, row, :], side[1, row, :], 2.0 * side[2, row, :], 2.0 * side[3, row, :]]
        for n, value in enumerate(values):
            for s in STRIPS:
                turned[n, a, s // STRIP] = turn(value, s)

    by_count(lambda n: whole_of(recv, n - 1, 0, 0).wait_recv())
    each(0, rows, lambda r: unpack(kinds, recv, 3 * blk_dev, r, r * blk_dev))
    spread_types(part_j)

    def tile_of(slot):
        first, second = tiles_ref[0, slot], tiles_ref[1, slot]
        return jnp.maximum(first, 0), jnp.maximum(second, 0), first

    def each_tile(sweep, first, want, begin=0, end=slots):
        most = min(want, max(64 // blocks_i, 1))
        group = max(g for g in range(1, most + 1) if begin % g == 0 and end % g == 0)

        def some(step, _):
            done = [sweep(step * group + k) for k in range(group)]
            for a in range(blocks_i):
                picks = [jnp.where(block == a, 1.0, 0.0) for block, _ in done]
                for n in range(len(done[0][1])):
                    place = pl.ds(((first + n) * blocks_i + a) * STRIP, STRIP)
                    level = acc[place, :]
                    for pick, (_, sums) in zip(picks, done):
                        level = level + pick * sums[n]
                    acc[place, :] = level
            return 0

        lax.fori_loop(begin // group, end // group, some, 0)

    def sent_row(k, block_j):
        return recv[lax.div(block_j, blk_dev), k * blk_dev + lax.rem(block_j, blk_dev)]

    def side_row(k, block_j):
        return wide(side[k, pl.ds(block_j, 1), :])

    same_atom = jnp.where(lax.broadcasted_iota(jnp.int32, (STRIP, TILE), 0) == 0, CUTOFF_SQ, 0.0)

    def born_sweep(slot):
        bi, bj, first = tile_of(slot)
        live = jnp.where(first >= 0, CUTOFF_SQ, 0.0)
        global_i = my_row * blocks_i + bi
        global_j = (lax.div(bj, blk_dev) * cols + my_col) * blk_dev + lax.rem(bj, blk_dev)
        self_pair = jnp.where(global_i == global_j, 1.0, 0.0)
        xj, yj, zj = (wide(sent_row(k, bj)) for k in range(3))
        gap_j = side_row(0, bj) + NECK_GAP
        vol_j, neck_j = side_row(2, bj), side_row(3, bj)
        born = None
        for s in STRIPS:
            span = pl.ds(s, STRIP)
            xi, yi, zi, rho_i, rho_sq = (turned[k, bi, s // STRIP] for k in range(5))
            dx, dy, dz = xi - xj, yi - yj, zi - zj
            q = dx * dx + dy * dy + dz * dz
            t = jnp.maximum((live if s else live - self_pair * same_atom) - q, 0.0)
            t_sq = t * t
            inv = 1.0 / (q + rho_sq)
            gap = rho_i + gap_j
            off = q - gap * gap
            bump = jnp.exp2(off * off * (-LOG2E / NECK_WIDTH))
            born = add(born, back(t_sq * (vol_j * inv * inv + neck_j * bump), s))
            geo[0, slot, span, :] = q
            geo[1, slot, span, :] = t
            geo[2, slot, span, :] = t_sq
            geo[3, slot, span, :] = bump
        return bi, [born]

    each_tile(born_sweep, 0, 16)

    def exchange(index, scale, piece, landing, channel):
        gathered = gather_up(index)
        for a in range(blocks_i):
            value = gathered[a : a + 1, :] * scale(a)
            piece[a] = value
            landing[my_col * blocks + blocks_j + a] = value
        for b in range(blk_dev):
            landing[my_col * blocks + my_row * blk_dev + b] = piece[my_col * blk_dev + b]

        def send(source, place, device):
            pltpu.make_async_remote_copy(
                source, landing.at[place], send_sem.at[channel], recv_sem.at[1 + channel],
                device_id=device, device_id_type=MESH,
            ).start()

        mine = pl.ds(my_col * blocks + my_row * blk_dev, blk_dev)

        def send_all(n):
            for dc in reversed(range(cols)):
                peer_col = wrap(my_col + dc, cols)
                source = piece.at[pl.ds(peer_col * blk_dev, blk_dev)]
                each_row(n, 0 if dc else 1, lambda r: send(source, mine, {"row": r, "col": peer_col}))

        by_count(send_all)
        own_row = pl.ds(my_col * blocks + blocks_j, blocks_i)
        each(1, cols, lambda s: send(piece, own_row, col_peer(s)))

        def all_of(n):
            return whole_of(landing, (n * cols - 1) * blk_dev + (cols - 1) * blocks_i, channel, 1 + channel)

        def finish():
            by_count(lambda n: all_of(n).wait_recv())

            def summed(b):
                value = landing[b]
                for c in range(1, cols):
                    value = value + landing[c * blocks + b]
                row = b if b < blocks_j else b + base_i - blocks_j
                total[row : row + 1, :] = value

            for b in range(blocks):
                summed(b)

        def drain():
            by_count(lambda n: all_of(n).wait_send())

        return finish, drain

    finish1, drain1 = exchange(0, lambda a: 1.0, part, partial_recv, 1)

    def slope_sweep(slot):
        bi, bj, _ = tile_of(slot)
        coords_j = [wide(sent_row(k, bj)) for k in range(3)]
        coords_i = [turned[k, bi, 0] for k in range(3)]
        gap_j = side_row(0, bj) + NECK_GAP
        rho_sq_j = side_row(1, bj)
        vol_j, neck_j = 2.0 * side_row(2, bj), 2.0 * side_row(3, bj)
        sums = [None] * 3
        for s in STRIPS:
            span = pl.ds(s, STRIP)
            rho_i, rho_sq, vol_i, neck_i = (turned[k, bi, s // STRIP] for k in range(3, 7))
            q, t, bump = geo[0, slot, span, :], geo[1, slot, span, :], geo[3, slot, span, :]
            soft_i, soft_j = q + rho_sq, q + rho_sq_j
            both = 1.0 / (soft_i * soft_j)
            inv_i, inv_j = both * soft_j, both * soft_i
            gap = rho_i + gap_j
            off = (q - gap * gap) * (1.0 / NECK_WIDTH)

            def slope(volume, neck, inv):
                far = volume * inv * inv
                near = neck * bump
                return t * (t * (far * inv + near * off) + (far + near))

            slope_ij = back(slope(vol_j, neck_j, inv_i), s)
            slope_ji = back(slope(vol_i, neck_i, inv_j), s)
            for k in range(3):
                d = coords_i[k] - back(coords_j[k], s)
                sums[k] = add(sums[k], slope_ij * d)
                geo[4 + k, slot, span, :] = d
                mom[k, slot, span, :] = slope_ji * d
        return bi, sums

    split = slots * EARLY_SLOPES // 32
    each_tile(slope_sweep, 1, 4, 0, split)
    alpha, beta, gamma = (by_type(kinds[...], k) for k in (3, 4, 5))
    by_count(lambda n: whole_of(recv_charge, n + cols - 2, 0, 5).wait_recv())
    each(0, rows, lambda r: unpack(charge, recv_charge, 0, r, r * blk_dev))
    for c in range(cols):
        unpack(charge, recv_charge, 0, rows + c, base_i + c * blk_dev)
    finish1()

    rho = side[0]
    scaled = rho * total[...]
    squash = jnp.tanh(
        alpha * scaled - beta * scaled * scaled + gamma * scaled * scaled * scaled
    )
    rad = 1.0 / (1.0 / rho - squash / (rho + OFFSET))
    radius[0] = rad
    radius[1] = (-0.25 * LOG2E) / rad
    radius[2] = rad * charge[...]
    for a in range(blocks_i):
        for s in STRIPS:
            strip = turn(rad[base_i + a : base_i + a + 1, :], s)
            turned_rad[0, a, s // STRIP] = strip
            turned_rad[1, a, s // STRIP] = 1.0 / strip

    def pair_sweep(slot):
        bi, bj, _ = tile_of(slot)
        rad_j, over_j, rad_charge_j = (wide(radius[k, pl.ds(bj, 1), :]) for k in range(3))
        grad = None
        for s in STRIPS:
            span = pl.ds(s, STRIP)
            q, t_sq = geo[0, slot, span, :], geo[2, slot, span, :]
            power = q * (turned_rad[1, bi, s // STRIP] * over_j)
            decay = jnp.exp2(power)
            inv = lax.rsqrt(q + turned_rad[0, bi, s // STRIP] * rad_j * decay)
            lean = t_sq * (inv * inv * inv)
            grad = add(grad, back(lean * (decay * (LOG2E - power)) * rad_charge_j, s))
            geo[2, slot, span, :] = inv
            geo[7, slot, span, :] = decay
        return bi, [grad]

    each_tile(pair_sweep, 4, 16)
    grad_scale = -0.5 / (CUTOFF_SQ * CUTOFF_SQ * LOG2E)
    finish2, drain2 = exchange(
        4, lambda a: grad_scale * charge[base_i + a : base_i + a + 1, :], grad_part, grad_recv, 2
    )

    def direct_sweep(slot):
        bi, bj, _ = tile_of(slot)
        charge_j = wide(charge[pl.ds(bj, 1), :])
        sums = [None] * 3
        for s in STRIPS:
            span = pl.ds(s, STRIP)
            t, inv, decay = (geo[k, slot, span, :] for k in (1, 2, 7))
            steep = t * inv
            pull = back(steep * charge_j * (2.0 + steep * inv * (0.5 - 0.125 * decay)), s)
            for k in range(3):
                sums[k] = add(sums[k], pull * geo[4 + k, slot, span, :])
        return bi, sums

    each_tile(slope_sweep, 1, 4, split, slots)
    each_tile(direct_sweep, 5, 4)
    early[0] = gather_up(1, 3)
    scaled = rho * total[...]
    squash = jnp.tanh(
        alpha * scaled - beta * scaled * scaled + gamma * scaled * scaled * scaled
    )
    rad = radius[0]
    slow = (
        COULOMB * rad * rad * (1.0 - squash * squash)
        * (alpha - 2.0 * beta * scaled + 3.0 * gamma * scaled * scaled)
        * rho / (rho + OFFSET)
    )
    rate[...] = slow
    chain_const[...] = (0.5 * charge[...] * charge[...] / (rad * rad)) * slow
    direct_scale = -2.0 * COULOMB / (CUTOFF_SQ * CUTOFF_SQ)
    gathered = gather_up(5, 3)
    charges_i = direct_scale * charge[base_i : base_i + blocks_i, :]
    early[1] = jnp.concatenate([charges_i] * 3, axis=0) * gathered
    finish2()
    chain[...] = chain_const[...] - rate[...] * total[...]

    def chain_sweep(slot):
        bi, bj, _ = tile_of(slot)
        base = wide(chain[pl.ds(bj, 1), :])
        sums = [None] * 3
        for s in STRIPS:
            span = pl.ds(s, STRIP)
            factor = back(base, s)
            for k in range(3):
                sums[k] = add(sums[k], factor * mom[k, slot, span, :])
        return bi, sums

    each_tile(chain_sweep, 8, 16)

    chain_i = jnp.concatenate([2.0 * chain[base_i : base_i + blocks_i, :]] * 3, axis=0)
    force = early[1] + chain_i * early[0] + 2.0 * gather_up(8, 3)
    for a in range(blocks_i):
        for k in range(3):
            row = k * blocks_i + a
            frc_part[a // blk_dev, k * blk_dev + a % blk_dev] = force[row : row + 1, :]

    for step in range(1, cols):
        peer_col = wrap(my_col + step, cols)
        pltpu.make_async_remote_copy(
            frc_part.at[peer_col], frc_recv.at[my_col], send_sem.at[3], recv_sem.at[4],
            device_id={"row": my_row, "col": peer_col}, device_id_type=MESH,
        ).start()
    frc_recv[my_col] = frc_part[my_col]
    by_count(lambda n: whole_of(recv, n + cols - 2, 0, 0).wait_send())
    by_count(lambda n: whole_of(recv_charge, n + cols - 2, 4, 5).wait_send())
    drain1()
    drain2()
    whole_of(frc_recv, cols - 1, 3, 4).wait_recv()
    for b in range(blk_dev):
        span = pl.ds(b * TILE, TILE)
        for k in range(3):
            value = frc_recv[0, k * blk_dev + b]
            for c in range(1, cols):
                value = value + frc_recv[c, k * blk_dev + b]
            out[1, k : k + 1, span] = value
            out[2, k : k + 1, span] = vel_ref[k : k + 1, span] + TIMESTEP / (2.0 * mass[b]) * (
                frc_ref[k : k + 1, span] + value
            )
    whole_of(frc_part, cols - 1, 3, 4).wait_send()


def solution(mesh):
    rows, cols = mesh.shape["row"], mesh.shape["col"]

    def body(positions, velocities, old_forces, charges, atom_types, type_table, tile_pairs):
        blk_dev = positions.shape[1] // TILE
        slots = tile_pairs.shape[-1]
        blocks_i, blocks_j = cols * blk_dev, rows * blk_dev
        blocks = -(-blocks_i // 8) * 8 + -(-blocks_j // 8) * 8
        landed = cols * (blocks_i + blocks_j)
        vmem = pl.BlockSpec(memory_space=pltpu.VMEM)
        anywhere = pl.BlockSpec(memory_space=pl.ANY)
        f32 = lambda *shape: pltpu.VMEM(shape, jnp.float32)
        dma = lambda n: pltpu.SemaphoreType.DMA((n,))
        out = pl.pallas_call(
            functools.partial(kernel, rows, cols, blk_dev),
            out_shape=pltpu.VMEM((3,) + positions.shape, jnp.float32),
            in_specs=[anywhere] * 7,
            out_specs=vmem,
            scratch_shapes=[
                pltpu.SMEM(type_table.shape, jnp.float32),
                pltpu.SMEM(tile_pairs.shape[2:], jnp.int32),
                f32(*positions.shape), f32(*positions.shape), f32(*positions.shape),
                f32(blk_dev, TILE),
                pltpu.VMEM((blk_dev, TILE), jnp.int32),
                dma(7),
                f32(SENT * blk_dev, 1, TILE),
                f32(rows + cols, SENT * blk_dev, 1, TILE),
                f32(blk_dev, 1, TILE),
                f32(rows + cols, blk_dev, 1, TILE),
                f32(blocks, TILE),
                f32(blocks, TILE),
                f32(4, blocks, TILE),
                f32(blocks, TILE),
                f32(3, blocks, TILE),
                f32(blocks, TILE),
                f32(blocks, TILE),
                f32(blocks, TILE),
                f32(7, blocks_i, TILE // STRIP, STRIP, TILE),
                f32(2, blocks_i, TILE // STRIP, STRIP, TILE),
                f32(8, slots, TILE, TILE),
                f32(3, slots, TILE, TILE),
                f32(11 * blocks_i * STRIP, TILE),
                f32(2, 3 * blocks_i, TILE),
                f32(blocks_i, 1, TILE),
                f32(landed, 1, TILE),
                f32(blocks_i, 1, TILE),
                f32(landed, 1, TILE),
                f32(cols, 3 * blk_dev, 1, TILE),
                f32(cols, 3 * blk_dev, 1, TILE),
                dma(5), dma(6),
            ],
            compiler_params=pltpu.CompilerParams(
                collective_id=0, has_side_effects=True, vmem_limit_bytes=60000 * 1024
            ),
            name="verlet",
        )(
            type_table, tile_pairs, positions, velocities, old_forces,
            charges.reshape(blk_dev, TILE), atom_types.reshape(blk_dev, TILE),
        )
        return out[0], out[2], out[1]

    return jax.shard_map(
        body,
        mesh=mesh,
        in_specs=(
            P(None, ("row", "col")),
            P(None, ("row", "col")),
            P(None, ("row", "col")),
            P(("row", "col")),
            P(("row", "col")),
            P(),
            P("row", "col", None, None),
        ),
        out_specs=(P(None, ("row", "col")), P(None, ("row", "col")), P(None, ("row", "col"))),
        check_vma=False,
    )
```

```python
import functools
import math

import jax
import jax.numpy as jnp
from jax import lax
from jax.experimental import pallas as pl
from jax.experimental.pallas import tpu as pltpu
from jax.sharding import PartitionSpec as P

TILE = 128
STRIP = 8
CUTOFF_SQ = 144.0
COULOMB = 32.0
TIMESTEP = 0.5
OFFSET = 0.09
NECK_GAP = 0.5
NECK_WIDTH = 16.0
LOG2E = math.log2(math.e)
MESH = pl.DeviceIdType.MESH
SENT = 4
STRIPS = range(0, TILE, STRIP)
UNROLL_PEERS = 32
EARLY_SLOPES = 24
CUTOFF = 12.0
DENSITY = 0.1


def near_rows(rows, row_blocks):
    side = round((rows * row_blocks) ** (1.0 / 3.0))
    side += side ** 3 < rows * row_blocks
    plane = side * side
    reach = int(CUTOFF / (TILE / DENSITY) ** (1.0 / 3.0)) + 1

    def interval(r):
        low = (r * row_blocks) // plane - reach
        high = ((r + 1) * row_blocks - 1) // plane + reach
        first = (jnp.maximum(low, 0) * plane) // row_blocks
        last = jnp.minimum(((high + 1) * plane - 1) // row_blocks, rows - 1)
        return first, last - first + 1

    with jax.ensure_compile_time_eval():
        counts = sorted({int(interval(r)[1]) for r in range(rows)})
    return interval, counts


def kernel(
    rows, cols, blk_dev, table_in, tiles_in, pos_in, vel_in, frc_in, chg_in, typ_in,
    out,
    table_ref, tiles_ref, pos_ref, vel_ref, frc_ref, chg_ref, typ_ref, load_sem,
    own, recv, own_charge, recv_charge, kinds, charge, side, total, radius, rate, chain_const, chain,
    turned, turned_rad, geo, mom, acc, early, part, partial_recv, grad_part, grad_recv, frc_part, frc_recv,
    send_sem, recv_sem,
):
    my_row, my_col = lax.axis_index("row"), lax.axis_index("col")
    blocks_j, blocks_i = rows * blk_dev, cols * blk_dev
    blocks = blocks_j + blocks_i
    base_i = total.shape[0] - -(-blocks_i // 8) * 8
    slots = tiles_ref.shape[1]
    types = table_ref.shape[1]

    def wrap(value, size):
        return jnp.where(value >= size, value - size, value)

    loads = [
        pltpu.make_async_copy(source, held, load_sem.at[k])
        for k, (source, held) in enumerate((
            (table_in, table_ref), (typ_in, typ_ref), (pos_in, pos_ref), (vel_in, vel_ref),
            (frc_in, frc_ref), (chg_in, chg_ref), (tiles_in.at[0, 0], tiles_ref),
        ))
    ]
    for load in loads:
        load.start()

    barrier = pltpu.get_barrier_semaphore()

    def each(first, last, action):
        if last - first <= UNROLL_PEERS:
            for step in range(first, last):
                action(step)
        else:
            def one(step, _):
                action(step)
                return 0

            lax.fori_loop(first, last, one, 0)

    interval, counts = near_rows(rows, blocks_i)
    first_row, row_count = interval(my_row)

    def by_count(action):
        if len(counts) == 1:
            action(counts[0])
        else:
            for n in counts:
                pl.when(row_count == n)(functools.partial(action, n))

    def each_row(n, first, action):
        part = max(rows // 4, 1)

        def at(step):
            action(first_row + wrap(my_row - first_row + step, n))

        each(min(2 * part, n), min(3 * part, n), at)
        each(min(part, n), min(2 * part, n), at)
        each(min(3 * part, n), n, at)
        each(first, min(part, n), at)

    def row_peer(peer_row):
        return {"row": peer_row, "col": my_col}

    def col_peer(step):
        return {"row": my_row, "col": wrap(my_col + step, cols)}

    def greet(device):
        pl.semaphore_signal(barrier, inc=1, device_id=device, device_id_type=MESH)

    by_count(lambda n: each_row(n, 1, lambda r: greet(row_peer(r))))
    each(1, cols, lambda s: greet(col_peer(s)))

    def clear_far(n):
        def clear(step):
            far = wrap(first_row + n + step, rows)
            recv[far] = jnp.zeros_like(recv[0])
            recv_charge[far] = jnp.zeros_like(recv_charge[0])
            for c in range(cols):
                for b in range(blk_dev):
                    place = c * blocks + far * blk_dev + b
                    partial_recv[place] = jnp.zeros((1, TILE), jnp.float32)
                    grad_recv[place] = jnp.zeros((1, TILE), jnp.float32)

        each(0, rows - n, clear)

    by_count(clear_far)

    for load in loads:
        load.wait()

    mass = []
    for b in range(blk_dev):
        span = pl.ds(b * TILE, TILE)
        kind = typ_ref[b : b + 1, :].astype(jnp.float32)
        m = jnp.zeros((1, TILE), jnp.float32)
        for t in range(types):
            m = jnp.where(kind == t, table_ref[6, t], m)
        mass.append(m)
        held = []
        for k in range(3):
            x = (
                pos_ref[k : k + 1, span]
                + TIMESTEP * vel_ref[k : k + 1, span]
                + TIMESTEP * TIMESTEP / (2.0 * m) * frc_ref[k : k + 1, span]
            )
            out[0, k : k + 1, span] = x
            held.append(x)
        for k, value in enumerate(held + [kind]):
            own[k * blk_dev + b] = value
            recv[my_row, k * blk_dev + b] = value
            recv[rows + my_col, k * blk_dev + b] = value
        value = chg_ref[b : b + 1, :]
        own_charge[b] = value
        recv_charge[my_row, b] = value
        recv_charge[rows + my_col, b] = value
    acc[...] = jnp.zeros_like(acc)
    kinds[...] = jnp.zeros_like(kinds)
    charge[...] = jnp.zeros_like(charge)
    total[...] = jnp.zeros_like(total)

    pl.semaphore_wait(barrier, row_count + cols - 2)

    def copy0(source, held, slot, send, receive, device):
        pltpu.make_async_remote_copy(
            source, held.at[slot], send_sem.at[send], recv_sem.at[receive],
            device_id=device, device_id_type=MESH,
        ).start()

    def copy0_rows(source, held, send, receive):
        by_count(lambda n: each_row(n, 1, lambda r: copy0(source, held, my_row, send, receive, row_peer(r))))

    def copy0_cols(source, held, send, receive):
        each(1, cols, lambda s: copy0(source, held, rows + my_col, send, receive, col_peer(s)))

    copy0_cols(own, recv, 0, 1)
    copy0_rows(own, recv, 0, 0)
    copy0_rows(own_charge, recv_charge, 4, 5)
    copy0_cols(own_charge, recv_charge, 4, 5)

    def whole_of(ref, count, send, receive):
        piece = ref.at[pl.ds(0, count)]
        return pltpu.make_async_remote_copy(
            piece, piece, send_sem.at[send], recv_sem.at[receive],
            device_id={"row": my_row, "col": my_col}, device_id_type=MESH,
        )

    def by_type(kind, row):
        value = jnp.full(kind.shape, table_ref[row, 0], jnp.float32)
        for t in range(1, types):
            value = jnp.where(kind == t, table_ref[row, t], value)
        return value

    def wide(value):
        return jnp.broadcast_to(value, (STRIP, TILE))

    def turn(value, s=0):
        return pltpu.roll(wide(value), s, 1, stride=1, stride_axis=0)

    def add(total_so_far, value):
        return value if total_so_far is None else total_so_far + value

    def back(value, s):
        return pltpu.roll(value, TILE - s, 1) if s else value

    def gather_up(first, count=1):
        held, level = count * blocks_i, None
        for r in range(STRIP):
            rows_r = acc[pl.ds(first * blocks_i * STRIP + r, held, stride=STRIP), :]
            level = add(level, back(rows_r, r))
        return level

    part_i, part_j = pl.ds(base_i, total.shape[0] - base_i), pl.ds(0, base_i)

    def spread_types(span):
        kind = kinds[span, :]
        rho = by_type(kind, 0)
        side[0, span, :] = rho
        side[1, span, :] = rho * rho
        side[2, span, :] = by_type(kind, 1) * rho * rho * rho * (1.0 / (CUTOFF_SQ * CUTOFF_SQ))
        side[3, span, :] = by_type(kind, 2) * (1.0 / (CUTOFF_SQ * CUTOFF_SQ))

    def unpack(held, source, first, slot, row):
        for b in range(blk_dev):
            held[pl.ds(row + b, 1), :] = source[slot, first + b]

    whole_of(recv, cols - 1, 0, 1).wait_recv()
    for c in range(cols):
        unpack(kinds, recv, 3 * blk_dev, rows + c, base_i + c * blk_dev)
    spread_types(part_i)
    def side_of(k, a):
        return side[k, base_i + a : base_i + a + 1, :]

    for a in range(blocks_i):
        c, b = a // blk_dev, a % blk_dev
        values = [recv[rows + c, k * blk_dev + b] for k in range(3)] + [side_of(0, a)]
        for s in STRIPS:
            for n, value in enumerate(values):
                turned[n, a, s // STRIP] = turn(value, s)
            rho_turned = turned[3, a, s // STRIP]
            turned[4, a, s // STRIP] = rho_turned * rho_turned

    by_count(lambda n: whole_of(recv, n - 1, 0, 0).wait_recv())
    each(0, rows, lambda r: unpack(kinds, recv, 3 * blk_dev, r, r * blk_dev))
    spread_types(part_j)

    def tile_of(slot):
        first, second = tiles_ref[0, slot], tiles_ref[1, slot]
        return jnp.maximum(first, 0), jnp.maximum(second, 0), first

    def each_tile(sweep, first, want, begin=0, end=slots):
        most = min(want, max(64 // blocks_i, 1))
        group = max(g for g in range(1, most + 1) if begin % g == 0 and end % g == 0)

        def some(step, _):
            done = [sweep(step * group + k) for k in range(group)]
            for a in range(blocks_i):
                picks = [jnp.where(block == a, 1.0, 0.0) for block, _ in done]
                for n in range(len(done[0][1])):
                    place = pl.ds(((first + n) * blocks_i + a) * STRIP, STRIP)
                    level = acc[place, :]
                    for pick, (_, sums) in zip(picks, done):
                        level = level + pick * sums[n]
                    acc[place, :] = level
            return 0

        lax.fori_loop(begin // group, end // group, some, 0)

    def sent_row(k, block_j):
        return recv[lax.div(block_j, blk_dev), k * blk_dev + lax.rem(block_j, blk_dev)]

    def side_row(k, block_j):
        return wide(side[k, pl.ds(block_j, 1), :])

    same_atom = jnp.where(lax.broadcasted_iota(jnp.int32, (STRIP, TILE), 0) == 0, CUTOFF_SQ, 0.0)

    def born_sweep(slot):
        bi, bj, first = tile_of(slot)
        live = jnp.where(first >= 0, CUTOFF_SQ, 0.0)
        global_i = my_row * blocks_i + bi
        global_j = (lax.div(bj, blk_dev) * cols + my_col) * blk_dev + lax.rem(bj, blk_dev)
        self_pair = jnp.where(global_i == global_j, 1.0, 0.0)
        xj, yj, zj = (wide(sent_row(k, bj)) for k in range(3))
        gap_j = side_row(0, bj) + NECK_GAP
        vol_j, neck_j = side_row(2, bj), side_row(3, bj)
        born = None
        for s in STRIPS:
            span = pl.ds(s, STRIP)
            xi, yi, zi, rho_i, rho_sq = (turned[k, bi, s // STRIP] for k in range(5))
            dx, dy, dz = xi - xj, yi - yj, zi - zj
            q = dx * dx + dy * dy + dz * dz
            t = jnp.maximum((live if s else live - self_pair * same_atom) - q, 0.0)
            t_sq = t * t
            inv = 1.0 / (q + rho_sq)
            gap = rho_i + gap_j
            off = q - gap * gap
            bump = jnp.exp2(off * off * (-LOG2E / NECK_WIDTH))
            born = add(born, back(t_sq * (vol_j * inv * inv + neck_j * bump), s))
            geo[0, slot, span, :] = q
            geo[1, slot, span, :] = t
            geo[2, slot, span, :] = t_sq
            geo[3, slot, span, :] = bump
        return bi, [born]

    each_tile(born_sweep, 0, 16)

    def exchange(index, scale, piece, landing, channel):
        gathered = gather_up(index)
        for a in range(blocks_i):
            value = gathered[a : a + 1, :] * scale(a)
            piece[a] = value
            landing[my_col * blocks + blocks_j + a] = value
        for b in range(blk_dev):
            landing[my_col * blocks + my_row * blk_dev + b] = piece[my_col * blk_dev + b]

        def send(source, place, device):
            pltpu.make_async_remote_copy(
                source, landing.at[place], send_sem.at[channel], recv_sem.at[1 + channel],
                device_id=device, device_id_type=MESH,
            ).start()

        mine = pl.ds(my_col * blocks + my_row * blk_dev, blk_dev)

        def send_all(n):
            for dc in reversed(range(cols)):
                peer_col = wrap(my_col + dc, cols)
                source = piece.at[pl.ds(peer_col * blk_dev, blk_dev)]
                each_row(n, 0 if dc else 1, lambda r: send(source, mine, {"row": r, "col": peer_col}))

        by_count(send_all)
        own_row = pl.ds(my_col * blocks + blocks_j, blocks_i)
        each(1, cols, lambda s: send(piece, own_row, col_peer(s)))

        def all_of(n):
            return whole_of(landing, (n * cols - 1) * blk_dev + (cols - 1) * blocks_i, channel, 1 + channel)

        def finish():
            by_count(lambda n: all_of(n).wait_recv())

            def summed(b):
                value = landing[b]
                for c in range(1, cols):
                    value = value + landing[c * blocks + b]
                row = b if b < blocks_j else b + base_i - blocks_j
                total[row : row + 1, :] = value

            for b in range(blocks):
                summed(b)

        def drain():
            by_count(lambda n: all_of(n).wait_send())

        return finish, drain

    finish1, drain1 = exchange(0, lambda a: 1.0, part, partial_recv, 1)

    for a in range(blocks_i):
        for s in STRIPS:
            for n in (2, 3):
                turned[3 + n, a, s // STRIP] = turn(2.0 * side_of(n, a), s)

    def slope_sweep(slot):
        bi, bj, _ = tile_of(slot)
        coords_j = [wide(sent_row(k, bj)) for k in range(3)]
        coords_i = [turned[k, bi, 0] for k in range(3)]
        gap_j = side_row(0, bj) + NECK_GAP
        rho_sq_j = side_row(1, bj)
        vol_j, neck_j = 2.0 * side_row(2, bj), 2.0 * side_row(3, bj)
        sums = [None] * 3
        for s in STRIPS:
            span = pl.ds(s, STRIP)
            rho_i, rho_sq, vol_i, neck_i = (turned[k, bi, s // STRIP] for k in range(3, 7))
            q, t, bump = geo[0, slot, span, :], geo[1, slot, span, :], geo[3, slot, span, :]
            soft_i, soft_j = q + rho_sq, q + rho_sq_j
            both = 1.0 / (soft_i * soft_j)
            inv_i, inv_j = both * soft_j, both * soft_i
            gap = rho_i + gap_j
            off = (q - gap * gap) * (1.0 / NECK_WIDTH)

            def slope(volume, neck, inv):
                far = volume * inv * inv
                near = neck * bump
                return t * (t * (far * inv + near * off) + (far + near))

            slope_ij = back(slope(vol_j, neck_j, inv_i), s)
            slope_ji = back(slope(vol_i, neck_i, inv_j), s)
            for k in range(3):
                d = coords_i[k] - back(coords_j[k], s)
                sums[k] = add(sums[k], slope_ij * d)
                geo[4 + k, slot, span, :] = d
                mom[k, slot, span, :] = slope_ji * d
        return bi, sums

    split = slots * EARLY_SLOPES // 32
    each_tile(slope_sweep, 1, 4, 0, split)
    alpha, beta, gamma = (by_type(kinds[...], k) for k in (3, 4, 5))
    by_count(lambda n: whole_of(recv_charge, n + cols - 2, 0, 5).wait_recv())
    each(0, rows, lambda r: unpack(charge, recv_charge, 0, r, r * blk_dev))
    for c in range(cols):
        unpack(charge, recv_charge, 0, rows + c, base_i + c * blk_dev)
    finish1()

    rho = side[0]
    scaled = rho * total[...]
    squash = jnp.tanh(
        alpha * scaled - beta * scaled * scaled + gamma * scaled * scaled * scaled
    )
    rad = 1.0 / (1.0 / rho - squash / (rho + OFFSET))
    radius[0] = rad
    radius[1] = (-0.25 * LOG2E) / rad
    radius[2] = rad * charge[...]
    for a in range(blocks_i):
        for s in STRIPS:
            strip = turn(rad[base_i + a : base_i + a + 1, :], s)
            turned_rad[0, a, s // STRIP] = strip
            turned_rad[1, a, s // STRIP] = 1.0 / strip

    def pair_sweep(slot):
        bi, bj, _ = tile_of(slot)
        rad_j, over_j, rad_charge_j = (wide(radius[k, pl.ds(bj, 1), :]) for k in range(3))
        grad = None
        for s in STRIPS:
            span = pl.ds(s, STRIP)
            q, t_sq = geo[0, slot, span, :], geo[2, slot, span, :]
            power = q * (turned_rad[1, bi, s // STRIP] * over_j)
            decay = jnp.exp2(power)
            inv = lax.rsqrt(q + turned_rad[0, bi, s // STRIP] * rad_j * decay)
            lean = t_sq * (inv * inv * inv)
            grad = add(grad, back(lean * (decay * (LOG2E - power)) * rad_charge_j, s))
            geo[2, slot, span, :] = inv
            geo[7, slot, span, :] = decay
        return bi, [grad]

    each_tile(pair_sweep, 4, 16)
    grad_scale = -0.5 / (CUTOFF_SQ * CUTOFF_SQ * LOG2E)
    finish2, drain2 = exchange(
        4, lambda a: grad_scale * charge[base_i + a : base_i + a + 1, :], grad_part, grad_recv, 2
    )

    def direct_sweep(slot):
        bi, bj, _ = tile_of(slot)
        charge_j = wide(charge[pl.ds(bj, 1), :])
        sums = [None] * 3
        for s in STRIPS:
            span = pl.ds(s, STRIP)
            t, inv, decay = (geo[k, slot, span, :] for k in (1, 2, 7))
            steep = t * inv
            pull = back(steep * charge_j * (2.0 + steep * inv * (0.5 - 0.125 * decay)), s)
            for k in range(3):
                sums[k] = add(sums[k], pull * geo[4 + k, slot, span, :])
        return bi, sums

    each_tile(slope_sweep, 1, 4, split, slots)
    each_tile(direct_sweep, 5, 4)
    early[0] = gather_up(1, 3)
    scaled = rho * total[...]
    squash = jnp.tanh(
        alpha * scaled - beta * scaled * scaled + gamma * scaled * scaled * scaled
    )
    rad = radius[0]
    slow = (
        COULOMB * rad * rad * (1.0 - squash * squash)
        * (alpha - 2.0 * beta * scaled + 3.0 * gamma * scaled * scaled)
        * rho / (rho + OFFSET)
    )
    rate[...] = slow
    chain_const[...] = (0.5 * charge[...] * charge[...] / (rad * rad)) * slow
    direct_scale = -2.0 * COULOMB / (CUTOFF_SQ * CUTOFF_SQ)
    gathered = gather_up(5, 3)
    charges_i = direct_scale * charge[base_i : base_i + blocks_i, :]
    early[1] = jnp.concatenate([charges_i] * 3, axis=0) * gathered
    finish2()
    chain[...] = chain_const[...] - rate[...] * total[...]

    def chain_sweep(slot):
        bi, bj, _ = tile_of(slot)
        base = wide(chain[pl.ds(bj, 1), :])
        sums = [None] * 3
        for s in STRIPS:
            span = pl.ds(s, STRIP)
            factor = back(base, s)
            for k in range(3):
                sums[k] = add(sums[k], factor * mom[k, slot, span, :])
        return bi, sums

    each_tile(chain_sweep, 8, 16)

    chain_i = jnp.concatenate([2.0 * chain[base_i : base_i + blocks_i, :]] * 3, axis=0)
    force = early[1] + chain_i * early[0] + 2.0 * gather_up(8, 3)
    for a in range(blocks_i):
        for k in range(3):
            row = k * blocks_i + a
            frc_part[a // blk_dev, k * blk_dev + a % blk_dev] = force[row : row + 1, :]

    for step in range(1, cols):
        peer_col = wrap(my_col + step, cols)
        pltpu.make_async_remote_copy(
            frc_part.at[peer_col], frc_recv.at[my_col], send_sem.at[3], recv_sem.at[4],
            device_id={"row": my_row, "col": peer_col}, device_id_type=MESH,
        ).start()
    frc_recv[my_col] = frc_part[my_col]
    by_count(lambda n: whole_of(recv, n + cols - 2, 0, 0).wait_send())
    by_count(lambda n: whole_of(recv_charge, n + cols - 2, 4, 5).wait_send())
    drain1()
    drain2()
    whole_of(frc_recv, cols - 1, 3, 4).wait_recv()
    for b in range(blk_dev):
        span = pl.ds(b * TILE, TILE)
        for k in range(3):
            value = frc_recv[0, k * blk_dev + b]
            for c in range(1, cols):
                value = value + frc_recv[c, k * blk_dev + b]
            out[1, k : k + 1, span] = value
            out[2, k : k + 1, span] = vel_ref[k : k + 1, span] + TIMESTEP / (2.0 * mass[b]) * (
                frc_ref[k : k + 1, span] + value
            )
    whole_of(frc_part, cols - 1, 3, 4).wait_send()


def solution(mesh):
    rows, cols = mesh.shape["row"], mesh.shape["col"]

    def body(positions, velocities, old_forces, charges, atom_types, type_table, tile_pairs):
        blk_dev = positions.shape[1] // TILE
        slots = tile_pairs.shape[-1]
        blocks_i, blocks_j = cols * blk_dev, rows * blk_dev
        blocks = -(-blocks_i // 8) * 8 + -(-blocks_j // 8) * 8
        landed = cols * (blocks_i + blocks_j)
        vmem = pl.BlockSpec(memory_space=pltpu.VMEM)
        anywhere = pl.BlockSpec(memory_space=pl.ANY)
        f32 = lambda *shape: pltpu.VMEM(shape, jnp.float32)
        dma = lambda n: pltpu.SemaphoreType.DMA((n,))
        out = pl.pallas_call(
            functools.partial(kernel, rows, cols, blk_dev),
            out_shape=pltpu.VMEM((3,) + positions.shape, jnp.float32),
            in_specs=[anywhere] * 7,
            out_specs=vmem,
            scratch_shapes=[
                pltpu.SMEM(type_table.shape, jnp.float32),
                pltpu.SMEM(tile_pairs.shape[2:], jnp.int32),
                f32(*positions.shape), f32(*positions.shape), f32(*positions.shape),
                f32(blk_dev, TILE),
                pltpu.VMEM((blk_dev, TILE), jnp.int32),
                dma(7),
                f32(SENT * blk_dev, 1, TILE),
                f32(rows + cols, SENT * blk_dev, 1, TILE),
                f32(blk_dev, 1, TILE),
                f32(rows + cols, blk_dev, 1, TILE),
                f32(blocks, TILE),
                f32(blocks, TILE),
                f32(4, blocks, TILE),
                f32(blocks, TILE),
                f32(3, blocks, TILE),
                f32(blocks, TILE),
                f32(blocks, TILE),
                f32(blocks, TILE),
                f32(7, blocks_i, TILE // STRIP, STRIP, TILE),
                f32(2, blocks_i, TILE // STRIP, STRIP, TILE),
                f32(8, slots, TILE, TILE),
                f32(3, slots, TILE, TILE),
                f32(11 * blocks_i * STRIP, TILE),
                f32(2, 3 * blocks_i, TILE),
                f32(blocks_i, 1, TILE),
                f32(landed, 1, TILE),
                f32(blocks_i, 1, TILE),
                f32(landed, 1, TILE),
                f32(cols, 3 * blk_dev, 1, TILE),
                f32(cols, 3 * blk_dev, 1, TILE),
                dma(5), dma(6),
            ],
            compiler_params=pltpu.CompilerParams(
                collective_id=0, has_side_effects=True, vmem_limit_bytes=60000 * 1024
            ),
            name="verlet",
        )(
            type_table, tile_pairs, positions, velocities, old_forces,
            charges.reshape(blk_dev, TILE), atom_types.reshape(blk_dev, TILE),
        )
        return out[0], out[2], out[1]

    return jax.shard_map(
        body,
        mesh=mesh,
        in_specs=(
            P(None, ("row", "col")),
            P(None, ("row", "col")),
            P(None, ("row", "col")),
            P(("row", "col")),
            P(("row", "col")),
            P(),
            P("row", "col", None, None),
        ),
        out_specs=(P(None, ("row", "col")), P(None, ("row", "col")), P(None, ("row", "col"))),
        check_vma=False,
    )
```
